32 devices in a mesh: snap: 4 (over y, x), vert: 8 (over z, core).
Axes of the slice: x: 2, y: 2, z: 4, core: 2. Of those that a mesh axis runs over, the one named last changes fastest.
Arguments:
- features: bfloat16 [32, 2048, 256], P('snap', 'vert'), may hold values from -6 to 6
- tile_cols: int32 [32, 16, 4], P('snap', 'vert'), may hold values from -1 to 15, as said below
- counts: int32 [32, 16], P('snap', 'vert'), may hold values from 1 to 4
- birth_snap: int32 [2048], P('vert'), may hold values from 0 to 31
- query_proj: bfloat16 [256, 256], replicated, may hold values from -0.375 to 0.375
- keyval_proj: bfloat16 [256, 512], replicated, may hold values from -0.375 to 0.375
- struct_out: bfloat16 [256, 256], replicated, may hold values from -0.375 to 0.375
- position_embedding_table: bfloat16 [32, 256], replicated, may hold values from -3 to 3
- temporal_qkv_weight: bfloat16 [256, 768], replicated, may hold values from -0.375 to 0.375
- temporal_output_weight: bfloat16 [256, 256], replicated, may hold values from -0.375 to 0.375
Outputs:
- embeddings: float32 [32, 8, 4, 64, 256], P(None, 'vert', 'snap')
The draws below stay inside these ranges and needn't reach their ends.
Inputs may be any that keep to these rules, and one draw needn't show every extreme that they name: `tile_cols`: entries k < counts[s, r] name column blocks of occupied tiles (a block may appear twice); the others are -1. Of the live entries of the 8 x 2 row blocks of one device, at most 10 lie in column blocks of any one index of vert, and exactly 10 for one index.
All inputs are finite; a program needn't handle non-finite values.
Results may differ from the reference program's by a relative error of at most 0.008.
Values may be sent and summed in bfloat16 or wider, within the bound.
No kernel may reach another device: no remote copies, remote signals or barrier semaphores. Data moves between devices by JAX's collectives and lax.ppermute only.
A program may use at most 128 MiB of HBM per device.

```python
import jax
import jax.numpy as jnp
from jax import lax

D = 256
HEADS = 8
TILE = 128
KT = 4
SNAP_DEV = 8
BLK_DEV = 2
S = 32
NB = 16
V = 2048
VQ = 64
N_SNAP = 4
N_VERT = 8


def tile_table(key):
    key = jax.random.fold_in(key, 7)
    key_counts, key_rest = jax.random.split(key)
    count_table = jax.random.randint(key_counts, (S, NB), 1, KT + 1).astype(jnp.int32)
    flat = SNAP_DEV * BLK_DEV * KT
    capacity = max(2, (flat + N_VERT - 2) // (N_VERT - 1))
    devices = N_SNAP * N_VERT
    per_device = count_table.reshape(N_SNAP, SNAP_DEV, N_VERT, BLK_DEV).transpose(0, 2, 1, 3).reshape(devices, SNAP_DEV * BLK_DEV)
    live = (jnp.arange(KT, dtype=jnp.int32)[None, None, :] < per_device[:, :, None]).reshape(devices, flat)
    device_keys = jax.random.split(key_rest, devices)

    def one_device(live_row, device_key):
        key_perm, key_hot, key_remainder, key_within = jax.random.split(device_key, 4)
        shuffle = jax.random.permutation(key_perm, flat).astype(jnp.int32)
        ranking = jnp.where(live_row, 0, flat).astype(jnp.int32) + shuffle
        ordering = jnp.argsort(ranking, stable=True).astype(jnp.int32)
        position = jnp.argsort(ordering, stable=True).astype(jnp.int32)
        busiest_tile = jax.random.randint(key_hot, (), 0, N_VERT).astype(jnp.int32)
        others = jax.random.permutation(key_remainder, N_VERT - 1).astype(jnp.int32)
        others = others + (others >= busiest_tile).astype(jnp.int32)
        owning_devices = jnp.where(position < capacity, busiest_tile, others[(position - capacity) % (N_VERT - 1)])
        within = jax.random.randint(key_within, (flat,), 0, BLK_DEV).astype(jnp.int32)
        return jnp.where(live_row, owning_devices * BLK_DEV + within, -1).astype(jnp.int32)
    columns = jax.vmap(one_device)(live, device_keys)
    columns = columns.reshape(N_SNAP, N_VERT, SNAP_DEV, BLK_DEV, KT).transpose(0, 2, 1, 3, 4).reshape(S, NB, KT)
    return (columns, count_table)


def draw_tile_cols(key, part):
    return tile_table(key)[0]


def draw_counts(key, part):
    return tile_table(key)[1]


def draw_features(key, part):
    key_base = jax.random.fold_in(key, 0)
    values = jax.random.truncated_normal(key_base, -6.0, 6.0, (S, V, D), jnp.float32)
    return values.astype(jnp.bfloat16)


def plant(drawn, stream_key, least, largest):
    spot = [jax.random.randint(jax.random.fold_in(stream_key, axis), (), 0, length) for axis, length in enumerate(drawn.shape)]
    widest = drawn.shape.index(max(drawn.shape))
    next_to = spot[:widest] + [(spot[widest] + 1) % drawn.shape[widest]] + spot[widest + 1:]
    return drawn.at[tuple(spot)].set(least).at[tuple(next_to)].set(largest)


def gaussian(key, extent, scale, bound, held_as=jnp.bfloat16):
    values = scale * jax.random.normal(key, extent, jnp.float32)
    return jnp.clip(values, min=-bound, max=bound).astype(held_as)


def setup_inputs(seed: int = 0) -> dict:
    keys = jax.random.split(jax.random.key(seed), 11)
    features = draw_features(jax.random.fold_in(keys[10], 71), 0)
    tile_cols = draw_tile_cols(jax.random.fold_in(keys[10], 71), 0)
    counts = draw_counts(jax.random.fold_in(keys[10], 71), 0)
    birth_snap = plant(jax.random.randint(keys[3], (V,), 0, S), jax.random.fold_in(keys[3], 1), 0, S - 1).astype(jnp.int32)
    query_proj = gaussian(keys[4], (D, D), D ** -0.5, 0.375)
    keyval_proj = gaussian(keys[5], (D, 2 * D), D ** -0.5, 0.375)
    struct_out = gaussian(keys[6], (D, D), D ** -0.5, 0.375)
    position_embedding_table = gaussian(keys[7], (S, D), 0.5, 3.0)
    temporal_qkv_weight = gaussian(keys[8], (D, 3 * D), D ** -0.5, 0.375)
    temporal_output_weight = gaussian(keys[9], (D, D), D ** -0.5, 0.375)
    return {"features": features, "tile_cols": tile_cols, "counts": counts, "birth_snap": birth_snap, "query_proj": query_proj, "keyval_proj": keyval_proj, "struct_out": struct_out, "position_embedding_table": position_embedding_table, "temporal_qkv_weight": temporal_qkv_weight, "temporal_output_weight": temporal_output_weight}


def attend_tiles(query_rows_all, key_rows, live_keys):
    count, span, model_width = query_rows_all.shape
    head_size = model_width // HEADS
    length = key_rows.shape[1]
    heads_q = query_rows_all.reshape(count, span, HEADS, head_size).astype(jnp.float32)
    keys_h = key_rows[:, :, :model_width].reshape(count, length, HEADS, head_size).astype(jnp.float32)
    values_h = key_rows[:, :, model_width:].reshape(count, length, HEADS, head_size).astype(jnp.float32)
    scores = jnp.einsum("bqhe,bkhe->bhqk", heads_q, keys_h) * (head_size ** -0.5)
    scores = jnp.where(live_keys[:, None, None, :], scores, -jnp.inf)
    weight_matrices = jax.nn.softmax(scores, axis=-1).astype(jnp.bfloat16)
    blended_rows = jnp.einsum("bhqk,bkhe->bqhe", weight_matrices.astype(jnp.float32), values_h)
    return blended_rows.astype(jnp.bfloat16).reshape(count, span, model_width)


def time_layer(hidden_block, births, position_embedding_table, temporal_qkv_weight, temporal_output_weight):
    length, count, model_width = hidden_block.shape
    head_size = model_width // HEADS
    blended_input = (hidden_block.astype(jnp.float32) + position_embedding_table.astype(jnp.float32)[:, None, :]).astype(jnp.bfloat16)
    projected_rows = jnp.einsum("mcf,fz->mcz", blended_input.astype(jnp.float32), temporal_qkv_weight.astype(jnp.float32)).astype(jnp.bfloat16)
    query_rows_all = projected_rows[:, :, :model_width].reshape(length, count, HEADS, head_size).astype(jnp.float32)
    keys_h = projected_rows[:, :, model_width:2 * model_width].reshape(length, count, HEADS, head_size).astype(jnp.float32)
    values_h = projected_rows[:, :, 2 * model_width:].reshape(length, count, HEADS, head_size).astype(jnp.float32)
    scores = jnp.einsum("snhe,tnhe->nhst", query_rows_all, keys_h) * (head_size ** -0.5)
    later = jnp.arange(length, dtype=jnp.int32)[:, None]
    earlier = jnp.arange(length, dtype=jnp.int32)[None, :]
    allowed = ((earlier <= later)[None] & (earlier[None] >= births[:, None, None])) | (earlier == later)[None]
    scores = jnp.where(allowed[:, None], scores, -jnp.inf)
    weight_matrices = jax.nn.softmax(scores, axis=-1).astype(jnp.bfloat16)
    blended_rows = jnp.einsum("nhst,tnhe->snhe", weight_matrices.astype(jnp.float32), values_h)
    blended_rows = blended_rows.astype(jnp.bfloat16).reshape(length, count, model_width)
    update_rows = jnp.einsum("mcf,fz->mcz", blended_rows.astype(jnp.float32), temporal_output_weight.astype(jnp.float32))
    return hidden_block.astype(jnp.float32) + update_rows


def reference(features, tile_cols, counts, birth_snap, query_proj, keyval_proj, struct_out, position_embedding_table, temporal_qkv_weight, temporal_output_weight):
    def snapshot(pieces):
        frame, cols, count_row = pieces
        query_rows_all = jnp.dot(frame, query_proj, preferred_element_type=jnp.float32).astype(jnp.bfloat16).reshape(NB, TILE, D)
        keyval = jnp.dot(frame, keyval_proj, preferred_element_type=jnp.float32).astype(jnp.bfloat16).reshape(NB, TILE, 2 * D)
        live_tiles = jnp.arange(KT, dtype=jnp.int32)[None, :] < count_row[:, None]
        index = jnp.where(live_tiles, cols, 0).astype(jnp.int32)
        key_rows = keyval[index].reshape(NB, KT * TILE, 2 * D)
        live_keys = jnp.repeat(live_tiles, TILE, axis=1)
        attended = attend_tiles(query_rows_all, key_rows, live_keys).reshape(V, D)
        update_rows = jnp.dot(attended, struct_out, preferred_element_type=jnp.float32)
        return (frame.astype(jnp.float32) + update_rows).astype(jnp.bfloat16)

    hidden = lax.map(snapshot, (features, tile_cols, counts))
    grouped = hidden.reshape(S, NB, TILE, D).transpose(1, 0, 2, 3)
    born = birth_snap.reshape(NB, TILE)

    def vertex_block(pieces):
        block, births = pieces
        return time_layer(block, births, position_embedding_table, temporal_qkv_weight, temporal_output_weight)

    result = lax.map(vertex_block, (grouped, born))
    result = result.transpose(1, 0, 2, 3).reshape(S, V, D)
    return result.reshape(S, N_VERT, N_SNAP, VQ, D)
```

```python
import functools
import math

import jax
import jax.numpy as jnp
from jax import lax
from jax.experimental import pallas as pl
from jax.experimental.pallas import tpu as pltpu
from jax.sharding import PartitionSpec as P

HEADS = 8
TILE = 128
CHUNKS = 2
F32 = jnp.float32
BF16 = jnp.bfloat16


def contract_last(a, b):
    return lax.dot_general(a, b, (((1,), (1,)), ((), ())), preferred_element_type=F32)


def matmul(a, b):
    return jnp.dot(a, b, preferred_element_type=F32)


def spread_heads(rows, head_size):
    column = lax.broadcasted_iota(jnp.int32, (1, rows.shape[1]), 1) // head_size
    return jnp.concatenate(
        [rows * (column == h).astype(BF16) for h in range(HEADS)], axis=0
    )


def gather_heads(low, high, count, head_size):
    parts = []
    for blended in (low, high):
        width = blended.shape[1] // 2
        column = lax.broadcasted_iota(jnp.int32, (1, width), 1) // head_size
        top = blended[:count, :width]
        bottom = blended[:count, width:]
        for h in range(1, HEADS // 2):
            rows = slice(h * count, (h + 1) * count)
            top = jnp.where(column == h, blended[rows, :width], top)
            bottom = jnp.where(column == h, blended[rows, width:], bottom)
        parts.append(top / bottom)
    return jnp.concatenate(parts, axis=1)


def structural_kernel(
    table_ref,
    offset_ref,
    x_ref,
    wq_ref,
    wkv_ref,
    wo_ref,
    out_ref,
    k_ref,
    v_ref,
    q_ref,
    s_ref,
    p_ref,
    a_ref,
    *,
    slots,
):
    pieces, piece_rows, width = x_ref.shape
    groups, peers, rows, _ = out_ref.shape
    half = width // 2
    head_size = width // HEADS
    total = pieces * piece_rows
    row_blocks = total // TILE
    block_rows = pieces * rows // row_blocks
    factor = head_size ** (-0.5) * math.log2(math.e)
    step = 2 * TILE
    pieces_per_step = step // piece_rows

    def project(i, carry):
        at = pl.ds(pl.multiple_of(i * step, step), step)
        x = x_ref[pl.ds(i * pieces_per_step, pieces_per_step)].reshape(step, width)
        keyval = matmul(x, wkv_ref[...]).astype(BF16)
        k_ref[at, :] = keyval[:, :width]
        ones = jnp.ones((step, half), BF16)
        v_ref[at, :] = jnp.concatenate(
            [keyval[:, width : width + half], ones, keyval[:, width + half :], ones], axis=1
        )
        return carry

    lax.fori_loop(0, total // step, project, 0)
    offset = pl.multiple_of(offset_ref[0], rows)
    x_rows = x_ref[:, pl.ds(offset, rows), :].reshape(pieces * rows, width)
    q_ref[...] = matmul(x_rows, wq_ref[...]).astype(BF16)

    def attend(r, tiles):
        count = table_ref[r * (slots + 1) + slots]
        at = pl.ds(pl.multiple_of(r * block_rows, block_rows), block_rows)
        spots = []
        for t in range(tiles):
            spot = jnp.maximum(table_ref[r * (slots + 1) + t], 0)
            spots.append(pl.ds(pl.multiple_of(spot * TILE, TILE), TILE))
        queries = spread_heads(q_ref[at, :], head_size)
        keys = jnp.concatenate([k_ref[spot, :] for spot in spots], axis=0)
        s_ref[:, : tiles * TILE] = contract_last(queries, keys)
        for h in range(HEADS):
            part = slice(h * block_rows, (h + 1) * block_rows)
            scores = []
            for t in range(tiles):
                score = s_ref[part, t * TILE : (t + 1) * TILE]
                if t == tiles - 1 and t > 0:
                    score = score + jnp.where(count > t, 0.0, -jnp.inf)
                scores.append(score)
            top = scores[0]
            for score in scores[1:]:
                top = jnp.maximum(top, score)
            top = jnp.max(top, axis=1, keepdims=True)
            for t in range(tiles):
                p_ref[part, t * TILE : (t + 1) * TILE] = jnp.exp2(
                    (scores[t] - top) * factor
                ).astype(BF16)
        values = jnp.concatenate([v_ref[spot, :] for spot in spots], axis=0)
        middle = HEADS // 2 * block_rows
        low = matmul(p_ref[:middle, : tiles * TILE], values[:, :width])
        high = matmul(p_ref[middle:, : tiles * TILE], values[:, width:])
        a_ref[at, :] = gather_heads(low, high, block_rows, head_size).astype(BF16)

    def row_block(r, carry):
        count = table_ref[r * (slots + 1) + slots]
        for tiles in range(2, slots + 1, 2):
            least = tiles - 2

            @pl.when((count > least) & (count <= tiles))
            def _(tiles=tiles):
                attend(r, tiles)

        return carry

    lax.fori_loop(0, row_blocks, row_block, 0)
    update = matmul(a_ref[...], wo_ref[...])
    hidden = (x_rows.astype(F32) + update).astype(BF16).reshape(peers, groups, rows, width)
    for g in range(groups):
        out_ref[g] = hidden[:, g]


def structural(table, offset, x, query_proj, keyval_proj, struct_out, rows, groups, slots):
    pieces, piece_rows, width = x.shape
    peers = pieces // groups
    total = pieces * piece_rows
    block_rows = TILE // piece_rows * rows
    vmem = pl.BlockSpec(memory_space=pltpu.VMEM)
    smem = pl.BlockSpec(memory_space=pltpu.SMEM)
    return pl.pallas_call(
        functools.partial(structural_kernel, slots=slots),
        out_shape=jax.ShapeDtypeStruct((groups, peers, rows, width), BF16),
        in_specs=[smem, smem, vmem, vmem, vmem, vmem],
        out_specs=vmem,
        scratch_shapes=[
            pltpu.VMEM((total, width), BF16),
            pltpu.VMEM((total, 2 * width), BF16),
            pltpu.VMEM((pieces * rows, width), BF16),
            pltpu.VMEM((HEADS * block_rows, slots * TILE), F32),
            pltpu.VMEM((HEADS * block_rows, slots * TILE), BF16),
            pltpu.VMEM((pieces * rows, width), BF16),
        ],
        compiler_params=pltpu.CompilerParams(vmem_limit_bytes=48 * 1024 * 1024),
        name="structural",
    )(table, offset, x, query_proj, keyval_proj, struct_out)


def temporal_kernel(h_ref, birth_ref, pos_ref, wt_ref, wo_ref, *refs):
    out_ref = refs[-1]
    length, count, width = h_ref.shape
    half = width // 2
    head_size = width // HEADS
    factor = head_size ** (-0.5) * math.log2(math.e)
    batch = min(count, 16)
    rows = batch * length
    together = max(1, TILE // length)
    span = together * length
    line = lax.broadcasted_iota(jnp.int32, (rows, rows), 0)
    column = lax.broadcasted_iota(jnp.int32, (rows, rows), 1)
    to_vertex = (
        (line // length == column % batch) & (line % length == column // batch)
    ).astype(BF16)
    to_time = (
        (line % batch == column // length) & (line // batch == column % length)
    ).astype(BF16)
    line = lax.broadcasted_iota(jnp.int32, (span, span), 0)
    column = lax.broadcasted_iota(jnp.int32, (span, span), 1)
    same = line // length == column // length
    before = same & (column < line)
    itself = line == column
    instant = lax.broadcasted_iota(jnp.int32, (1, span), 1) % length
    ones = jnp.ones((span, half), BF16)
    positions = pos_ref[...].astype(F32)[:, None, :]
    for b in range(count // batch):
        part = slice(b * batch, (b + 1) * batch)
        hidden = h_ref[:, part, :].astype(F32)
        time_in = (hidden + positions).astype(BF16).reshape(rows, width)
        time_in = matmul(to_vertex, time_in).astype(BF16)
        projected = matmul(time_in, wt_ref[...]).astype(BF16)
        mixed = []
        for g in range(batch // together):
            at = slice(g * span, (g + 1) * span)
            queries = spread_heads(projected[at, :width], head_size)
            values = projected[at, 2 * width :]
            scores = contract_last(queries, projected[at, width : 2 * width])
            index = b * (batch // together) + g
            alive = instant >= birth_ref[index : index + 1, :]
            kept = itself | (before & alive)
            weights = []
            for h in range(HEADS):
                score = jnp.where(kept, scores[h * span : (h + 1) * span], -jnp.inf)
                top = jnp.max(score, axis=1, keepdims=True)
                weights.append(jnp.exp2((score - top) * factor).astype(BF16))
            low = jnp.concatenate(weights[: HEADS // 2], axis=0)
            high = jnp.concatenate(weights[HEADS // 2 :], axis=0)
            low = matmul(low, jnp.concatenate([values[:, :half], ones], axis=1))
            high = matmul(high, jnp.concatenate([values[:, half:], ones], axis=1))
            mixed.append(gather_heads(low, high, span, head_size).astype(BF16))
        mixed = jnp.concatenate(mixed, axis=0)
        mixed = matmul(to_time, mixed).astype(BF16)
        update = matmul(mixed, wo_ref[...]).reshape(length, batch, width)
        out_ref[:, part, :] = hidden + update


def temporal(hidden, births, positions, qkv_weight, output_weight, total, chunk, earlier):
    length, count, width = hidden.shape
    vmem = pl.BlockSpec(memory_space=pltpu.VMEM)
    args = [hidden, births, positions, qkv_weight, output_weight]
    specs = [pl.BlockSpec(a.shape, lambda i, n=a.ndim: (0,) * n) for a in args]
    aliases = {}
    if earlier is not None:
        aliases = {len(args): 0}
        args.append(earlier)
        specs.append(pl.BlockSpec(memory_space=pl.ANY))
    return pl.pallas_call(
        temporal_kernel,
        grid=(1,),
        out_shape=jax.ShapeDtypeStruct((length, total, width), F32),
        in_specs=specs,
        out_specs=pl.BlockSpec((length, count, width), lambda i: (0, chunk, 0)),
        input_output_aliases=aliases,
        compiler_params=pltpu.CompilerParams(vmem_limit_bytes=48 * 1024 * 1024),
        name="temporal",
    )(*args)


def local(
    features,
    tile_cols,
    counts,
    birth_snap,
    query_proj,
    keyval_proj,
    struct_out,
    position_embedding_table,
    temporal_qkv_weight,
    temporal_output_weight,
):
    snap_count, vert_rows, width = features.shape
    slots = tile_cols.shape[2]
    peers = lax.axis_size("vert")
    groups = lax.axis_size("snap")
    snapshots = snap_count * groups
    quarter = vert_rows // groups
    sharers = peers // snap_count
    chunks = max(1, min(CHUNKS, quarter // (sharers * 16)))
    rows = quarter // (sharers * chunks)

    table = jnp.concatenate([tile_cols, counts[:, :, None]], axis=2)
    outgoing = features
    if sharers > 1:
        outgoing = jnp.repeat(features, sharers, axis=0)
        table = jnp.repeat(table, sharers, axis=0)
    snapshot = lax.all_to_all(outgoing, "vert", split_axis=0, concat_axis=0, tiled=True)
    table = lax.all_to_all(table, "vert", split_axis=0, concat_axis=0, tiled=True).reshape(-1)
    x = snapshot.reshape(peers * groups, quarter, width)
    share = lax.axis_index("vert") % sharers

    arrived = []
    for c in range(chunks):
        offset = jnp.reshape((c * sharers + share) * rows, (1,)).astype(jnp.int32)
        hidden = structural(
            table, offset, x, query_proj, keyval_proj, struct_out, rows, groups, slots
        )
        hidden = hidden.reshape(groups * peers, rows, width)
        hidden = lax.all_to_all(
            hidden, ("snap", "vert"), split_axis=0, concat_axis=0, tiled=True
        )
        arrived.append(hidden.reshape(snapshots, sharers * rows, width))

    births = lax.dynamic_slice_in_dim(birth_snap, lax.axis_index("snap") * quarter, quarter)
    span = max(1, TILE // snapshots) * snapshots
    births = jnp.repeat(births, snapshots).reshape(chunks, -1, span)
    result = None
    for c in range(chunks):
        result = temporal(
            arrived[c],
            births[c],
            position_embedding_table,
            temporal_qkv_weight,
            temporal_output_weight,
            quarter,
            c,
            result,
        )
    return result[:, None, None]


def solution(mesh):
    placed = (
        P("snap", "vert", None),
        P("snap", "vert", None),
        P("snap", "vert"),
        P("vert"),
        P(),
        P(),
        P(),
        P(),
        P(),
        P(),
    )
    return jax.shard_map(
        local,
        mesh=mesh,
        in_specs=placed,
        out_specs=P(None, "vert", "snap", None, None),
        check_vma=False,
    )
```

```python
import functools
import math

import jax
import jax.numpy as jnp
from jax import lax
from jax.experimental import pallas as pl
from jax.experimental.pallas import tpu as pltpu
from jax.sharding import PartitionSpec as P

HEADS = 8
TILE = 128
CHUNKS = 2
F32 = jnp.float32
BF16 = jnp.bfloat16


def contract_last(a, b):
    return lax.dot_general(a, b, (((1,), (1,)), ((), ())), preferred_element_type=F32)


def matmul(a, b):
    return jnp.dot(a, b, preferred_element_type=F32)


def spread_heads(rows, head_size):
    column = lax.broadcasted_iota(jnp.int32, (1, rows.shape[1]), 1) // head_size
    return jnp.concatenate(
        [rows * (column == h).astype(BF16) for h in range(HEADS)], axis=0
    )


def gather_heads(low, high, count, head_size):
    parts = []
    for blended in (low, high):
        width = blended.shape[1] // 2
        column = lax.broadcasted_iota(jnp.int32, (1, width), 1) // head_size
        top = blended[:count, :width]
        bottom = blended[:count, width:]
        for h in range(1, HEADS // 2):
            rows = slice(h * count, (h + 1) * count)
            top = jnp.where(column == h, blended[rows, :width], top)
            bottom = jnp.where(column == h, blended[rows, width:], bottom)
        parts.append(top / bottom)
    return jnp.concatenate(parts, axis=1)


def structural_kernel(
    table_ref,
    offset_ref,
    x_ref,
    wq_ref,
    wkv_ref,
    wo_ref,
    out_ref,
    k_ref,
    v_ref,
    q_ref,
    s_ref,
    p_ref,
    a_ref,
    *,
    slots,
):
    pieces, piece_rows, width = x_ref.shape
    groups, peers, rows, _ = out_ref.shape
    half = width // 2
    head_size = width // HEADS
    total = pieces * piece_rows
    row_blocks = total // TILE
    block_rows = pieces * rows // row_blocks
    factor = head_size ** (-0.5) * math.log2(math.e)
    step = 2 * TILE
    pieces_per_step = step // piece_rows

    def project(i, carry):
        at = pl.ds(pl.multiple_of(i * step, step), step)
        x = x_ref[pl.ds(i * pieces_per_step, pieces_per_step)].reshape(step, width)
        keyval = matmul(x, wkv_ref[...]).astype(BF16)
        k_ref[at, :] = keyval[:, :width]
        ones = jnp.ones((step, half), BF16)
        v_ref[at, :] = jnp.concatenate(
            [keyval[:, width : width + half], ones, keyval[:, width + half :], ones], axis=1
        )
        return carry

    lax.fori_loop(0, total // step, project, 0)
    offset = pl.multiple_of(offset_ref[0], rows)
    x_rows = x_ref[:, pl.ds(offset, rows), :].reshape(pieces * rows, width)
    q_ref[...] = matmul(x_rows, wq_ref[...]).astype(BF16)

    def attend(r, tiles):
        count = table_ref[r * (slots + 1) + slots]
        at = pl.ds(pl.multiple_of(r * block_rows, block_rows), block_rows)
        spots = []
        for t in range(tiles):
            spot = jnp.maximum(table_ref[r * (slots + 1) + t], 0)
            spots.append(pl.ds(pl.multiple_of(spot * TILE, TILE), TILE))
        queries = spread_heads(q_ref[at, :], head_size)
        keys = jnp.concatenate([k_ref[spot, :] for spot in spots], axis=0)
        s_ref[:, : tiles * TILE] = contract_last(queries, keys)
        for h in range(HEADS):
            part = slice(h * block_rows, (h + 1) * block_rows)
            scores = []
            for t in range(tiles):
                score = s_ref[part, t * TILE : (t + 1) * TILE]
                if t == tiles - 1 and t > 0:
                    score = score + jnp.where(count > t, 0.0, -jnp.inf)
                scores.append(score)
            top = scores[0]
            for score in scores[1:]:
                top = jnp.maximum(top, score)
            top = jnp.max(top, axis=1, keepdims=True)
            for t in range(tiles):
                p_ref[part, t * TILE : (t + 1) * TILE] = jnp.exp2(
                    (scores[t] - top) * factor
                ).astype(BF16)
        values = jnp.concatenate([v_ref[spot, :] for spot in spots], axis=0)
        middle = HEADS // 2 * block_rows
        low = matmul(p_ref[:middle, : tiles * TILE], values[:, :width])
        high = matmul(p_ref[middle:, : tiles * TILE], values[:, width:])
        a_ref[at, :] = gather_heads(low, high, block_rows, head_size).astype(BF16)

    def row_block(r, carry):
        count = table_ref[r * (slots + 1) + slots]
        for tiles in range(2, slots + 1, 2):
            least = tiles - 2

            @pl.when((count > least) & (count <= tiles))
            def _(tiles=tiles):
                attend(r, tiles)

        return carry

    lax.fori_loop(0, row_blocks, row_block, 0)
    update = matmul(a_ref[...], wo_ref[...])
    hidden = (x_rows.astype(F32) + update).astype(BF16).reshape(peers, groups, rows, width)
    for g in range(groups):
        out_ref[g] = hidden[:, g]


def structural(table, offset, x, query_proj, keyval_proj, struct_out, rows, groups, slots):
    pieces, piece_rows, width = x.shape
    peers = pieces // groups
    total = pieces * piece_rows
    block_rows = TILE // piece_rows * rows
    vmem = pl.BlockSpec(memory_space=pltpu.VMEM)
    smem = pl.BlockSpec(memory_space=pltpu.SMEM)
    return pl.pallas_call(
        functools.partial(structural_kernel, slots=slots),
        out_shape=jax.ShapeDtypeStruct((groups, peers, rows, width), BF16),
        in_specs=[smem, smem, vmem, vmem, vmem, vmem],
        out_specs=vmem,
        scratch_shapes=[
            pltpu.VMEM((total, width), BF16),
            pltpu.VMEM((total, 2 * width), BF16),
            pltpu.VMEM((pieces * rows, width), BF16),
            pltpu.VMEM((HEADS * block_rows, slots * TILE), F32),
            pltpu.VMEM((HEADS * block_rows, slots * TILE), BF16),
            pltpu.VMEM((pieces * rows, width), BF16),
        ],
        compiler_params=pltpu.CompilerParams(vmem_limit_bytes=48 * 1024 * 1024),
        name="structural",
    )(table, offset, x, query_proj, keyval_proj, struct_out)


def temporal_kernel(h_ref, birth_ref, pos_ref, wt_ref, wo_ref, *refs):
    out_ref = refs[-1]
    length, count, width = h_ref.shape
    half = width // 2
    head_size = width // HEADS
    factor = head_size ** (-0.5) * math.log2(math.e)
    batch = min(count, 16)
    rows = batch * length
    together = max(1, TILE // length)
    span = together * length
    line = lax.broadcasted_iota(jnp.int32, (rows, rows), 0)
    column = lax.broadcasted_iota(jnp.int32, (rows, rows), 1)
    to_vertex = (
        (line // length == column % batch) & (line % length == column // batch)
    ).astype(BF16)
    to_time = (
        (line % batch == column // length) & (line // batch == column % length)
    ).astype(BF16)
    line = lax.broadcasted_iota(jnp.int32, (span, span), 0)
    column = lax.broadcasted_iota(jnp.int32, (span, span), 1)
    same = line // length == column // length
    before = same & (column < line)
    itself = line == column
    instant = lax.broadcasted_iota(jnp.int32, (1, span), 1) % length
    ones = jnp.ones((span, half), BF16)
    positions = pos_ref[...].astype(F32)[:, None, :]
    for b in range(count // batch):
        part = slice(b * batch, (b + 1) * batch)
        hidden = h_ref[:, part, :].astype(F32)
        time_in = (hidden + positions).astype(BF16).reshape(rows, width)
        time_in = matmul(to_vertex, time_in).astype(BF16)
        projected = matmul(time_in, wt_ref[...]).astype(BF16)
        mixed = []
        for g in range(batch // together):
            at = slice(g * span, (g + 1) * span)
            queries = spread_heads(projected[at, :width], head_size)
            values = projected[at, 2 * width :]
            scores = contract_last(queries, projected[at, width : 2 * width])
            index = b * (batch // together) + g
            alive = instant >= birth_ref[index : index + 1, :]
            kept = itself | (before & alive)
            weights = []
            for h in range(HEADS):
                score = jnp.where(kept, scores[h * span : (h + 1) * span], -jnp.inf)
                top = jnp.max(score, axis=1, keepdims=True)
                weights.append(jnp.exp2((score - top) * factor).astype(BF16))
            low = jnp.concatenate(weights[: HEADS // 2], axis=0)
            high = jnp.concatenate(weights[HEADS // 2 :], axis=0)
            low = matmul(low, jnp.concatenate([values[:, :half], ones], axis=1))
            high = matmul(high, jnp.concatenate([values[:, half:], ones], axis=1))
            mixed.append(gather_heads(low, high, span, head_size).astype(BF16))
        mixed = jnp.concatenate(mixed, axis=0)
        mixed = matmul(to_time, mixed).astype(BF16)
        update = matmul(mixed, wo_ref[...]).reshape(length, batch, width)
        out_ref[:, part, :] = hidden + update


def temporal(hidden, births, positions, qkv_weight, output_weight, total, chunk, earlier):
    length, count, width = hidden.shape
    vmem = pl.BlockSpec(memory_space=pltpu.VMEM)
    args = [hidden, births, positions, qkv_weight, output_weight]
    specs = [pl.BlockSpec(a.shape, lambda i, n=a.ndim: (0,) * n) for a in args]
    aliases = {}
    if earlier is not None:
        aliases = {len(args): 0}
        args.append(earlier)
        specs.append(pl.BlockSpec(memory_space=pl.ANY))
    return pl.pallas_call(
        temporal_kernel,
        grid=(1,),
        out_shape=jax.ShapeDtypeStruct((length, total, width), F32),
        in_specs=specs,
        out_specs=pl.BlockSpec((length, count, width), lambda i: (0, chunk, 0)),
        input_output_aliases=aliases,
        compiler_params=pltpu.CompilerParams(vmem_limit_bytes=48 * 1024 * 1024),
        name="temporal",
    )(*args)


def local(
    features,
    tile_cols,
    counts,
    birth_snap,
    query_proj,
    keyval_proj,
    struct_out,
    position_embedding_table,
    temporal_qkv_weight,
    temporal_output_weight,
):
    snap_count, vert_rows, width = features.shape
    slots = tile_cols.shape[2]
    peers = lax.axis_size("vert")
    groups = lax.axis_size("snap")
    snapshots = snap_count * groups
    quarter = vert_rows // groups
    sharers = peers // snap_count
    chunks = max(1, min(CHUNKS, quarter // (sharers * 16)))
    rows = quarter // (sharers * chunks)

    table = jnp.concatenate([tile_cols, counts[:, :, None]], axis=2)
    outgoing = features
    if sharers > 1:
        outgoing = jnp.repeat(features, sharers, axis=0)
    snapshot = lax.all_to_all(outgoing, "vert", split_axis=0, concat_axis=0, tiled=True)
    tables = lax.all_gather(table, "vert", axis=1)
    own = lax.axis_index("vert") // sharers
    table = lax.dynamic_index_in_dim(tables, own, 0, keepdims=False).reshape(-1)
    x = snapshot.reshape(peers * groups, quarter, width)
    share = lax.axis_index("vert") % sharers

    arrived = []
    for c in range(chunks):
        offset = jnp.reshape((c * sharers + share) * rows, (1,)).astype(jnp.int32)
        hidden = structural(
            table, offset, x, query_proj, keyval_proj, struct_out, rows, groups, slots
        )
        hidden = hidden.reshape(groups * peers, rows, width)
        hidden = lax.all_to_all(
            hidden, ("snap", "vert"), split_axis=0, concat_axis=0, tiled=True
        )
        arrived.append(hidden.reshape(snapshots, sharers * rows, width))

    births = lax.dynamic_slice_in_dim(birth_snap, lax.axis_index("snap") * quarter, quarter)
    span = max(1, TILE // snapshots) * snapshots
    births = jnp.repeat(births, snapshots).reshape(chunks, -1, span)
    result = None
    for c in range(chunks):
        result = temporal(
            arrived[c],
            births[c],
            position_embedding_table,
            temporal_qkv_weight,
            temporal_output_weight,
            quarter,
            c,
            result,
        )
    return result[:, None, None]


def solution(mesh):
    placed = (
        P("snap", "vert", None),
        P("snap", "vert", None),
        P("snap", "vert"),
        P("vert"),
        P(),
        P(),
        P(),
        P(),
        P(),
        P(),
    )
    return jax.shard_map(
        local,
        mesh=mesh,
        in_specs=placed,
        out_specs=P(None, "vert", "snap", None, None),
        check_vma=False,
    )
```

```python
import functools
import math

import jax
import jax.numpy as jnp
from jax import lax
from jax.experimental import pallas as pl
from jax.experimental.pallas import tpu as pltpu
from jax.sharding import PartitionSpec as P

HEADS = 8
TILE = 128
CHUNKS = 2
TOGETHER = 16
F32 = jnp.float32
BF16 = jnp.bfloat16


def contract_last(a, b):
    return lax.dot_general(a, b, (((1,), (1,)), ((), ())), preferred_element_type=F32)


def matmul(a, b):
    return jnp.dot(a, b, preferred_element_type=F32)


def spread_heads(rows, head_size):
    column = lax.broadcasted_iota(jnp.int32, (1, rows.shape[1]), 1) // head_size
    return jnp.concatenate(
        [rows * (column == h).astype(BF16) for h in range(HEADS)], axis=0
    )


def gather_heads(low, high, count, head_size):
    parts = []
    for blended in (low, high):
        width = blended.shape[1] // 2
        column = lax.broadcasted_iota(jnp.int32, (1, width), 1) // head_size
        top = blended[:count, :width]
        bottom = blended[:count, width:]
        for h in range(1, HEADS // 2):
            rows = slice(h * count, (h + 1) * count)
            top = jnp.where(column == h, blended[rows, :width], top)
            bottom = jnp.where(column == h, blended[rows, width:], bottom)
        parts.append(top / bottom)
    return jnp.concatenate(parts, axis=1)


def structural_kernel(
    offset_ref,
    x_ref,
    wq_ref,
    wk_ref,
    wvt_ref,
    wo_ref,
    out_ref,
    k_ref,
    v_ref,
    q_ref,
    s_ref,
    p_ref,
    a_ref,
    loaded_ref,
    table_ref,
    table_sem,
    *,
    slots,
):
    peers, _, width = x_ref.shape
    groups, _, rows, _ = out_ref.shape
    total = k_ref.shape[0]
    vert_rows = total // peers
    quarter = vert_rows // groups
    half = width // 2
    half_heads = HEADS // 2
    head_size = width // HEADS
    blocks = vert_rows // TILE
    row_blocks = total // TILE
    pieces = TILE // quarter
    span = pieces * rows
    lanes = half_heads * span
    units = s_ref.shape[0]
    merged = min(blocks, 128 // span)
    factor = head_size ** (-0.5) * math.log2(math.e)
    for i in range(peers):
        tail = x_ref[i, vert_rows:, :128].astype(F32)
        loaded_ref[i : i + 1, :] = tail[:1].astype(jnp.int32)
    load = pltpu.make_async_copy(loaded_ref, table_ref, table_sem)
    load.start()

    def project(i, carry):
        at = pl.ds(pl.multiple_of(i * vert_rows, vert_rows), vert_rows)
        x = x_ref[i, :vert_rows, :]
        k_ref[at, :] = matmul(x, wk_ref[...]).astype(BF16)
        values = contract_last(wvt_ref[...], x).astype(BF16)
        v_ref[0, :half, at] = values[:half]
        v_ref[1, :half, at] = values[half:]
        return carry

    lax.fori_loop(0, peers, project, 0, unroll=2)
    v_ref[:, half:, :total] = jnp.ones((2, v_ref.shape[1] - half, total), BF16)
    v_ref[:, :, total:] = jnp.zeros((2, v_ref.shape[1], TILE), BF16)
    offset = pl.multiple_of(offset_ref[0], rows)
    for g in range(groups):
        x_rows = x_ref[:, pl.ds(offset + g * quarter, rows), :].reshape(peers * rows, width)
        q_ref[g] = (
            (matmul(x_rows, wq_ref[...]) * factor).astype(BF16).reshape(peers, rows, width)
        )

    load.wait()

    def read_slots(peer, block):
        base = block * (slots + 1)
        count = table_ref[peer, base + slots]
        first = table_ref[peer, base]
        keys = []
        values = []
        for t in range(slots):
            spot = table_ref[peer, base + t]
            key = jnp.where(count > t, spot, first)
            value = jnp.where(count > t, spot, row_blocks)
            keys.append(pl.ds(pl.multiple_of(key * TILE, TILE), TILE))
            values.append(pl.ds(pl.multiple_of(value * TILE, TILE), TILE))
        return keys, values

    def score(unit, peer, block):
        keys, _ = read_slots(peer, block)
        queries = jnp.concatenate(
            [q_ref[block * pieces + i, peer] for i in range(pieces)], axis=0
        )
        keys = jnp.concatenate([k_ref[key, :] for key in keys], axis=0)
        s_ref[unit] = contract_last(keys, spread_heads(queries, head_size))

    def blend(unit, peer, block):
        _, values = read_slots(peer, block)
        parts = []
        for j in range(2):
            for c in range(j * lanes, (j + 1) * lanes, 128):
                top = jnp.max(s_ref[unit, :, c : c + 128], axis=0, keepdims=True)
                p_ref[unit, :, c : c + 128] = jnp.exp2(
                    s_ref[unit, :, c : c + 128] - top
                ).astype(BF16)
            value = jnp.concatenate([v_ref[j, :, spot] for spot in values], axis=1)
            mixed = matmul(value, p_ref[unit, :, j * lanes : (j + 1) * lanes])
            for h in range(half_heads):
                c = h * span // 128 * 128
                part = mixed[h * head_size : (h + 1) * head_size, c : c + 128]
                part = part / mixed[half : half + 1, c : c + 128]
                shift = (block % merged - h) * span % 128
                if shift:
                    part = pltpu.roll(part, shift, 1)
                parts.append(part)
        return jnp.concatenate(parts, axis=0)

    def some_peers(i, carry):
        todo = [(p, b) for p in range(units // blocks) for b in range(blocks)]
        lane = lax.broadcasted_iota(jnp.int32, (1, 128), 1) // span
        score(0, i * (units // blocks), 0)
        wide = None
        for n, (p, b) in enumerate(todo):
            if n + 1 < len(todo):
                score(n + 1, i * (units // blocks) + todo[n + 1][0], todo[n + 1][1])
            peer = i * (units // blocks) + p
            part = blend(n, peer, b)
            wide = part if b % merged == 0 else jnp.where(lane == b % merged, part, wide)
            if b % merged == merged - 1:
                narrow = wide.T[: merged * span].astype(BF16)
                for n in range(merged * pieces):
                    g = (b + 1 - merged) * pieces + n
                    a_ref[g, peer] = narrow[n * rows : (n + 1) * rows]
        return carry

    lax.fori_loop(0, row_blocks // units, some_peers, 0)
    for g in range(groups):
        update = matmul(a_ref[g].reshape(peers * rows, width), wo_ref[...])
        x_rows = x_ref[:, pl.ds(offset + g * quarter, rows), :].reshape(peers * rows, width)
        hidden = (x_rows.astype(F32) + update).astype(BF16)
        out_ref[g] = hidden.reshape(peers, rows, width)


def structural(offset, x, query_proj, keyval_proj, struct_out, vert_rows, rows, groups, slots):
    peers, _, width = x.shape
    total = peers * vert_rows
    span = TILE // (vert_rows // groups) * rows
    vmem = pl.BlockSpec(memory_space=pltpu.VMEM)
    smem = pl.BlockSpec(memory_space=pltpu.SMEM)
    return pl.pallas_call(
        functools.partial(structural_kernel, slots=slots),
        out_shape=jax.ShapeDtypeStruct((groups, peers, rows, width), BF16),
        in_specs=[smem, vmem, vmem, vmem, vmem, vmem],
        out_specs=vmem,
        scratch_shapes=[
            pltpu.VMEM((total, width), BF16),
            pltpu.VMEM((2, width // 2 + 16, total + TILE), BF16),
            pltpu.VMEM((groups, peers, rows, width), BF16),
            pltpu.VMEM((TOGETHER, slots * TILE, HEADS * span), F32),
            pltpu.VMEM((TOGETHER, slots * TILE, HEADS * span), BF16),
            pltpu.VMEM((groups, peers, rows, width), BF16),
            pltpu.VMEM((peers, 128), jnp.int32),
            pltpu.SMEM((peers, 128), jnp.int32),
            pltpu.SemaphoreType.DMA,
        ],
        compiler_params=pltpu.CompilerParams(vmem_limit_bytes=48 * 1024 * 1024),
        name="structural",
    )(
        offset,
        x,
        query_proj,
        keyval_proj[:, :width],
        keyval_proj[:, width:].T,
        struct_out,
    )


def temporal_kernel(h_ref, birth_ref, pos_ref, wt_ref, wo_ref, *refs):
    out_ref = refs[-1]
    length, count, width = h_ref.shape
    half = width // 2
    head_size = width // HEADS
    factor = head_size ** (-0.5) * math.log2(math.e)
    batch = min(count, 16)
    rows = batch * length
    together = max(1, TILE // length)
    span = together * length
    line = lax.broadcasted_iota(jnp.int32, (rows, rows), 0)
    column = lax.broadcasted_iota(jnp.int32, (rows, rows), 1)
    to_vertex = (
        (line // length == column % batch) & (line % length == column // batch)
    ).astype(BF16)
    to_time = (
        (line % batch == column // length) & (line // batch == column % length)
    ).astype(BF16)
    line = lax.broadcasted_iota(jnp.int32, (span, span), 0)
    column = lax.broadcasted_iota(jnp.int32, (span, span), 1)
    same = line // length == column // length
    before = same & (column < line)
    itself = line == column
    instant = lax.broadcasted_iota(jnp.int32, (1, span), 1) % length
    ones = jnp.ones((span, half), BF16)
    positions = pos_ref[...].astype(F32)[:, None, :]
    for b in range(count // batch):
        part = slice(b * batch, (b + 1) * batch)
        hidden = h_ref[:, part, :].astype(F32)
        time_in = (hidden + positions).astype(BF16).reshape(rows, width)
        time_in = matmul(to_vertex, time_in).astype(BF16)
        projected = matmul(time_in, wt_ref[...]).astype(BF16)
        mixed = []
        for g in range(batch // together):
            at = slice(g * span, (g + 1) * span)
            queries = spread_heads(projected[at, :width], head_size)
            values = projected[at, 2 * width :]
            scores = contract_last(queries, projected[at, width : 2 * width])
            index = b * (batch // together) + g
            alive = instant >= birth_ref[index : index + 1, :]
            kept = itself | (before & alive)
            weights = []
            for h in range(HEADS):
                score = jnp.where(kept, scores[h * span : (h + 1) * span], -jnp.inf)
                top = jnp.max(score, axis=1, keepdims=True)
                weights.append(jnp.exp2((score - top) * factor).astype(BF16))
            low = jnp.concatenate(weights[: HEADS // 2], axis=0)
            high = jnp.concatenate(weights[HEADS // 2 :], axis=0)
            low = matmul(low, jnp.concatenate([values[:, :half], ones], axis=1))
            high = matmul(high, jnp.concatenate([values[:, half:], ones], axis=1))
            mixed.append(gather_heads(low, high, span, head_size).astype(BF16))
        mixed = jnp.concatenate(mixed, axis=0)
        mixed = matmul(to_time, mixed).astype(BF16)
        update = matmul(mixed, wo_ref[...]).reshape(length, batch, width)
        out_ref[:, part, :] = hidden + update


def temporal(hidden, births, positions, qkv_weight, output_weight, total, chunk, earlier):
    length, count, width = hidden.shape
    vmem = pl.BlockSpec(memory_space=pltpu.VMEM)
    args = [hidden, births, positions, qkv_weight, output_weight]
    specs = [pl.BlockSpec(a.shape, lambda i, n=a.ndim: (0,) * n) for a in args]
    aliases = {}
    if earlier is not None:
        aliases = {len(args): 0}
        args.append(earlier)
        specs.append(pl.BlockSpec(memory_space=pl.ANY))
    return pl.pallas_call(
        temporal_kernel,
        grid=(1,),
        out_shape=jax.ShapeDtypeStruct((length, total, width), F32),
        in_specs=specs,
        out_specs=pl.BlockSpec((length, count, width), lambda i: (0, chunk, 0)),
        input_output_aliases=aliases,
        compiler_params=pltpu.CompilerParams(vmem_limit_bytes=48 * 1024 * 1024),
        name="temporal",
    )(*args)


def local(
    features,
    tile_cols,
    counts,
    birth_snap,
    query_proj,
    keyval_proj,
    struct_out,
    position_embedding_table,
    temporal_qkv_weight,
    temporal_output_weight,
):
    snap_count, vert_rows, width = features.shape
    slots = tile_cols.shape[2]
    peers = lax.axis_size("vert")
    groups = lax.axis_size("snap")
    snapshots = snap_count * groups
    quarter = vert_rows // groups
    sharers = peers // snap_count
    chunks = max(1, min(CHUNKS, quarter // (sharers * 16)))
    rows = quarter // (sharers * chunks)

    table = jnp.concatenate([tile_cols, counts[:, :, None]], axis=2).astype(BF16)
    table = table.reshape(snap_count, 1, -1)
    table = jnp.pad(table, ((0, 0), (0, 15), (0, width - table.shape[2])))
    outgoing = jnp.concatenate([features, table], axis=1)
    if sharers > 1:
        outgoing = jnp.repeat(outgoing, sharers, axis=0)
    x = lax.all_to_all(outgoing, "vert", split_axis=0, concat_axis=0, tiled=True)
    share = lax.axis_index("vert") % sharers

    arrived = []
    for c in range(chunks):
        offset = jnp.reshape((c * sharers + share) * rows, (1,)).astype(jnp.int32)
        hidden = structural(
            offset, x, query_proj, keyval_proj, struct_out, vert_rows, rows, groups, slots
        )
        hidden = hidden.reshape(groups * peers, rows, width)
        hidden = lax.all_to_all(
            hidden, ("snap", "vert"), split_axis=0, concat_axis=0, tiled=True
        )
        arrived.append(hidden.reshape(snapshots, sharers * rows, width))

    births = lax.dynamic_slice_in_dim(birth_snap, lax.axis_index("snap") * quarter, quarter)
    span = max(1, TILE // snapshots) * snapshots
    births = jnp.repeat(births, snapshots).reshape(chunks, -1, span)
    result = None
    for c in range(chunks):
        result = temporal(
            arrived[c],
            births[c],
            position_embedding_table,
            temporal_qkv_weight,
            temporal_output_weight,
            quarter,
            c,
            result,
        )
    return result[:, None, None]


def solution(mesh):
    placed = (
        P("snap", "vert", None),
        P("snap", "vert", None),
        P("snap", "vert"),
        P("vert"),
        P(),
        P(),
        P(),
        P(),
        P(),
        P(),
    )
    return jax.shard_map(
        local,
        mesh=mesh,
        in_specs=placed,
        out_specs=P(None, "vert", "snap", None, None),
        check_vma=False,
    )
```

```python
import functools
import math

import jax
import jax.numpy as jnp
from jax import lax
from jax.experimental import pallas as pl
from jax.experimental.pallas import tpu as pltpu
from jax.sharding import PartitionSpec as P

HEADS = 8
TILE = 128
CHUNKS = 2
TOGETHER = 16
F32 = jnp.float32
BF16 = jnp.bfloat16


def contract_last(a, b):
    return lax.dot_general(a, b, (((1,), (1,)), ((), ())), preferred_element_type=F32)


def matmul(a, b):
    return jnp.dot(a, b, preferred_element_type=F32)


def spread_heads(rows, head_size):
    column = lax.broadcasted_iota(jnp.int32, (1, rows.shape[1]), 1) // head_size
    return jnp.concatenate(
        [rows * (column == h).astype(BF16) for h in range(HEADS)], axis=0
    )


def gather_heads(low, high, count, head_size):
    parts = []
    for blended in (low, high):
        width = blended.shape[1] // 2
        column = lax.broadcasted_iota(jnp.int32, (1, width), 1) // head_size
        top = blended[:count, :width]
        bottom = blended[:count, width:]
        for h in range(1, HEADS // 2):
            rows = slice(h * count, (h + 1) * count)
            top = jnp.where(column == h, blended[rows, :width], top)
            bottom = jnp.where(column == h, blended[rows, width:], bottom)
        parts.append(top / bottom)
    return jnp.concatenate(parts, axis=1)


def pack_kernel(features_ref, cols_ref, counts_ref, *refs, sharers):
    slab_refs, sems = refs[:-1], refs[-1]
    peers = len(slab_refs)
    _, vert_rows, width = features_ref.shape
    _, blocks, slots = cols_ref.shape
    me = lax.axis_index("vert")
    lane = lax.broadcasted_iota(jnp.int32, (slab_refs[0].shape[0] - vert_rows, width), 1)
    copies = []
    for i, slab in enumerate(slab_refs):
        own = lax.rem(me + i, peers) // sharers
        copy = pltpu.make_async_copy(
            features_ref.at[own], slab.at[pl.ds(0, vert_rows), :], sems.at[i]
        )
        copy.start()
        copies.append(copy)
    for i, slab in enumerate(slab_refs):
        own = lax.rem(me + i, peers) // sharers
        table = jnp.zeros(lane.shape, jnp.int32)
        for b in range(blocks):
            base = b * (slots + 1)
            for t in range(slots):
                table = jnp.where(lane == base + t, cols_ref[own, b, t], table)
            table = jnp.where(lane == base + slots, counts_ref[own, b], table)
        slab[vert_rows:, :] = table.astype(F32).astype(BF16)
    for copy in copies:
        copy.wait()


def pack(features, tile_cols, counts, peers, sharers):
    _, vert_rows, width = features.shape
    smem = pl.BlockSpec(memory_space=pltpu.SMEM)
    vmem = pl.BlockSpec(memory_space=pltpu.VMEM)
    slab = jax.ShapeDtypeStruct((vert_rows + 16, width), BF16)
    return list(
        pl.pallas_call(
            functools.partial(pack_kernel, sharers=sharers),
            out_shape=[slab] * peers,
            in_specs=[pl.BlockSpec(memory_space=pl.ANY), smem, smem],
            out_specs=[vmem] * peers,
            scratch_shapes=[pltpu.SemaphoreType.DMA((peers,))],
            name="pack",
        )(features, tile_cols, counts)
    )


def structural_kernel(
    place_ref,
    wq_ref,
    wk_ref,
    wvt_ref,
    wo_ref,
    *refs,
    slots,
):
    slab_refs, rest = refs[:-10], refs[-10:]
    out_ref, k_ref, v_ref, q_ref, s_ref, p_ref, a_ref, loaded_ref, table_ref, table_sem = rest
    groups, peers, rows, width = out_ref.shape
    total = k_ref.shape[0]
    vert_rows = total // peers
    quarter = vert_rows // groups
    half = width // 2
    half_heads = HEADS // 2
    head_size = width // HEADS
    blocks = vert_rows // TILE
    row_blocks = total // TILE
    pieces = TILE // quarter
    span = pieces * rows
    lanes = half_heads * span
    units = s_ref.shape[0]
    merged = min(blocks, 128 // span)
    factor = head_size ** (-0.5) * math.log2(math.e)
    offset = pl.multiple_of(place_ref[0], rows)
    senders = [lax.rem(place_ref[1] + peers - i, peers) for i in range(peers)]
    for sender, slab in zip(senders, slab_refs):
        tail = slab[vert_rows:, :128].astype(F32)
        loaded_ref[pl.ds(sender, 1), :] = tail[:1].astype(jnp.int32)
    load = pltpu.make_async_copy(loaded_ref, table_ref, table_sem)
    load.start()

    def query_rows(slab):
        return jnp.concatenate(
            [slab[pl.ds(offset + g * quarter, rows), :] for g in range(groups)], axis=0
        )

    v_ref[:, half:, :total] = jnp.ones((2, v_ref.shape[1] - half, total), BF16)
    v_ref[:, :, total:] = jnp.zeros((2, v_ref.shape[1], TILE), BF16)
    for sender, slab in zip(senders, slab_refs):
        at = pl.ds(pl.multiple_of(sender * vert_rows, vert_rows), vert_rows)
        x = slab[:vert_rows, :]
        k_ref[at, :] = matmul(x, wk_ref[...]).astype(BF16)
        values = contract_last(wvt_ref[...], x).astype(BF16)
        v_ref[0, :half, at] = values[:half]
        v_ref[1, :half, at] = values[half:]
        queries = (matmul(query_rows(slab), wq_ref[...]) * factor).astype(BF16)
        for g in range(groups):
            q_ref[g, sender] = queries[g * rows : (g + 1) * rows]
    load.wait()

    def read_slots(peer, block):
        base = block * (slots + 1)
        count = table_ref[peer, base + slots]
        first = table_ref[peer, base]
        keys = []
        values = []
        for t in range(slots):
            spot = table_ref[peer, base + t]
            key = jnp.where(count > t, spot, first)
            value = jnp.where(count > t, spot, row_blocks)
            keys.append(pl.ds(pl.multiple_of(key * TILE, TILE), TILE))
            values.append(pl.ds(pl.multiple_of(value * TILE, TILE), TILE))
        return keys, values

    def score(unit, peer, block):
        keys, _ = read_slots(peer, block)
        queries = jnp.concatenate(
            [q_ref[block * pieces + i, peer] for i in range(pieces)], axis=0
        )
        keys = jnp.concatenate([k_ref[key, :] for key in keys], axis=0)
        s_ref[unit] = contract_last(keys, spread_heads(queries, head_size))

    def blend(unit, peer, block):
        _, values = read_slots(peer, block)
        parts = []
        for j in range(2):
            for c in range(j * lanes, (j + 1) * lanes, 128):
                top = jnp.max(s_ref[unit, :, c : c + 128], axis=0, keepdims=True)
                p_ref[unit, :, c : c + 128] = jnp.exp2(
                    s_ref[unit, :, c : c + 128] - top
                ).astype(BF16)
            value = jnp.concatenate([v_ref[j, :, spot] for spot in values], axis=1)
            mixed = matmul(value, p_ref[unit, :, j * lanes : (j + 1) * lanes])
            for h in range(half_heads):
                c = h * span // 128 * 128
                part = mixed[h * head_size : (h + 1) * head_size, c : c + 128]
                part = part / mixed[half : half + 1, c : c + 128]
                shift = (block % merged - h) * span % 128
                if shift:
                    part = pltpu.roll(part, shift, 1)
                parts.append(part)
        return jnp.concatenate(parts, axis=0)

    def some_peers(i, carry):
        todo = [(p, b) for p in range(units // blocks) for b in range(blocks)]
        lane = lax.broadcasted_iota(jnp.int32, (1, 128), 1) // span
        score(0, i * (units // blocks), 0)
        wide = None
        for n, (p, b) in enumerate(todo):
            if n + 1 < len(todo):
                score(n + 1, i * (units // blocks) + todo[n + 1][0], todo[n + 1][1])
            peer = i * (units // blocks) + p
            part = blend(n, peer, b)
            wide = part if b % merged == 0 else jnp.where(lane == b % merged, part, wide)
            if b % merged == merged - 1:
                narrow = wide.T[: merged * span].astype(BF16)
                for n in range(merged * pieces):
                    g = (b + 1 - merged) * pieces + n
                    a_ref[g, peer] = narrow[n * rows : (n + 1) * rows]
        return carry

    lax.fori_loop(0, row_blocks // units, some_peers, 0)
    for sender, slab in zip(senders, slab_refs):
        mixed = jnp.concatenate([a_ref[g, sender] for g in range(groups)], axis=0)
        hidden = query_rows(slab).astype(F32) + matmul(mixed, wo_ref[...])
        for g in range(groups):
            out_ref[g, sender] = hidden[g * rows : (g + 1) * rows].astype(BF16)


def structural(place, slabs, query_proj, keyval_proj, struct_out, vert_rows, rows, groups, slots):
    peers = len(slabs)
    width = slabs[0].shape[1]
    total = peers * vert_rows
    span = TILE // (vert_rows // groups) * rows
    vmem = pl.BlockSpec(memory_space=pltpu.VMEM)
    smem = pl.BlockSpec(memory_space=pltpu.SMEM)
    return pl.pallas_call(
        functools.partial(structural_kernel, slots=slots),
        out_shape=jax.ShapeDtypeStruct((groups, peers, rows, width), BF16),
        in_specs=[smem] + [vmem] * (4 + peers),
        out_specs=vmem,
        scratch_shapes=[
            pltpu.VMEM((total, width), BF16),
            pltpu.VMEM((2, width // 2 + 16, total + TILE), BF16),
            pltpu.VMEM((groups, peers, rows, width), BF16),
            pltpu.VMEM((TOGETHER, slots * TILE, HEADS * span), F32),
            pltpu.VMEM((TOGETHER, slots * TILE, HEADS * span), BF16),
            pltpu.VMEM((groups, peers, rows, width), BF16),
            pltpu.VMEM((peers, 128), jnp.int32),
            pltpu.SMEM((peers, 128), jnp.int32),
            pltpu.SemaphoreType.DMA,
        ],
        compiler_params=pltpu.CompilerParams(vmem_limit_bytes=48 * 1024 * 1024),
        name="structural",
    )(
        place,
        query_proj,
        keyval_proj[:, :width],
        keyval_proj[:, width:].T,
        struct_out,
        *slabs,
    )


def temporal_kernel(h_ref, birth_ref, pos_ref, wt_ref, wo_ref, *refs):
    out_ref = refs[-1]
    length, count, width = h_ref.shape
    half = width // 2
    head_size = width // HEADS
    factor = head_size ** (-0.5) * math.log2(math.e)
    batch = min(count, 16)
    rows = batch * length
    together = max(1, TILE // length)
    span = together * length
    line = lax.broadcasted_iota(jnp.int32, (rows, rows), 0)
    column = lax.broadcasted_iota(jnp.int32, (rows, rows), 1)
    to_vertex = (
        (line // length == column % batch) & (line % length == column // batch)
    ).astype(BF16)
    to_time = (
        (line % batch == column // length) & (line // batch == column % length)
    ).astype(BF16)
    line = lax.broadcasted_iota(jnp.int32, (span, span), 0)
    column = lax.broadcasted_iota(jnp.int32, (span, span), 1)
    same = line // length == column // length
    before = same & (column < line)
    itself = line == column
    instant = lax.broadcasted_iota(jnp.int32, (1, span), 1) % length
    ones = jnp.ones((span, half), BF16)
    positions = pos_ref[...].astype(F32)[:, None, :]
    for b in range(count // batch):
        part = slice(b * batch, (b + 1) * batch)
        hidden = h_ref[:, part, :].astype(F32)
        time_in = (hidden + positions).astype(BF16).reshape(rows, width)
        time_in = matmul(to_vertex, time_in).astype(BF16)
        projected = matmul(time_in, wt_ref[...]).astype(BF16)
        mixed = []
        for g in range(batch // together):
            at = slice(g * span, (g + 1) * span)
            queries = spread_heads(projected[at, :width], head_size)
            values = projected[at, 2 * width :]
            scores = contract_last(queries, projected[at, width : 2 * width])
            index = b * (batch // together) + g
            alive = instant >= birth_ref[index : index + 1, :]
            kept = itself | (before & alive)
            weights = []
            for h in range(HEADS):
                score = jnp.where(kept, scores[h * span : (h + 1) * span], -jnp.inf)
                top = jnp.max(score, axis=1, keepdims=True)
                weights.append(jnp.exp2((score - top) * factor).astype(BF16))
            low = jnp.concatenate(weights[: HEADS // 2], axis=0)
            high = jnp.concatenate(weights[HEADS // 2 :], axis=0)
            low = matmul(low, jnp.concatenate([values[:, :half], ones], axis=1))
            high = matmul(high, jnp.concatenate([values[:, half:], ones], axis=1))
            mixed.append(gather_heads(low, high, span, head_size).astype(BF16))
        mixed = jnp.concatenate(mixed, axis=0)
        mixed = matmul(to_time, mixed).astype(BF16)
        update = matmul(mixed, wo_ref[...]).reshape(length, batch, width)
        out_ref[:, part, :] = hidden + update


def temporal(hidden, births, positions, qkv_weight, output_weight, total, chunk, earlier):
    length, count, width = hidden.shape
    vmem = pl.BlockSpec(memory_space=pltpu.VMEM)
    args = [hidden, births, positions, qkv_weight, output_weight]
    specs = [pl.BlockSpec(a.shape, lambda i, n=a.ndim: (0,) * n) for a in args]
    aliases = {}
    if earlier is not None:
        aliases = {len(args): 0}
        args.append(earlier)
        specs.append(pl.BlockSpec(memory_space=pl.ANY))
    return pl.pallas_call(
        temporal_kernel,
        grid=(1,),
        out_shape=jax.ShapeDtypeStruct((length, total, width), F32),
        in_specs=specs,
        out_specs=pl.BlockSpec((length, count, width), lambda i: (0, chunk, 0)),
        input_output_aliases=aliases,
        compiler_params=pltpu.CompilerParams(vmem_limit_bytes=48 * 1024 * 1024),
        name="temporal",
    )(*args)


def local(
    features,
    tile_cols,
    counts,
    birth_snap,
    query_proj,
    keyval_proj,
    struct_out,
    position_embedding_table,
    temporal_qkv_weight,
    temporal_output_weight,
):
    snap_count, vert_rows, width = features.shape
    slots = tile_cols.shape[2]
    peers = lax.axis_size("vert")
    groups = lax.axis_size("snap")
    snapshots = snap_count * groups
    quarter = vert_rows // groups
    sharers = peers // snap_count
    chunks = max(1, min(CHUNKS, quarter // (sharers * 16)))
    rows = quarter // (sharers * chunks)

    me = lax.axis_index("vert")
    share = me % sharers
    slabs = pack(features, tile_cols, counts, peers, sharers)
    for i in range(1, peers):
        slabs[i] = lax.ppermute(slabs[i], "vert", [(v, (v + i) % peers) for v in range(peers)])

    arrived = []
    for c in range(chunks):
        place = jnp.stack([(c * sharers + share) * rows, me]).astype(jnp.int32)
        hidden = structural(
            place, slabs, query_proj, keyval_proj, struct_out, vert_rows, rows, groups, slots
        )
        hidden = hidden.reshape(groups * peers, rows, width)
        hidden = lax.all_to_all(
            hidden, ("snap", "vert"), split_axis=0, concat_axis=0, tiled=True
        )
        arrived.append(hidden.reshape(snapshots, sharers * rows, width))

    births = lax.dynamic_slice_in_dim(birth_snap, lax.axis_index("snap") * quarter, quarter)
    span = max(1, TILE // snapshots) * snapshots
    births = jnp.repeat(births, snapshots).reshape(chunks, -1, span)
    result = None
    for c in range(chunks):
        result = temporal(
            arrived[c],
            births[c],
            position_embedding_table,
            temporal_qkv_weight,
            temporal_output_weight,
            quarter,
            c,
            result,
        )
    return result[:, None, None]


def solution(mesh):
    placed = (
        P("snap", "vert", None),
        P("snap", "vert", None),
        P("snap", "vert"),
        P("vert"),
        P(),
        P(),
        P(),
        P(),
        P(),
        P(),
    )
    return jax.shard_map(
        local,
        mesh=mesh,
        in_specs=placed,
        out_specs=P(None, "vert", "snap", None, None),
        check_vma=False,
    )
```

```python
import functools
import math

import jax
import jax.numpy as jnp
from jax import lax
from jax.experimental import pallas as pl
from jax.experimental.pallas import tpu as pltpu
from jax.sharding import PartitionSpec as P

HEADS = 8
TILE = 128
EXTRA = 8
CHUNKS = 2
TOGETHER = 16
F32 = jnp.float32
BF16 = jnp.bfloat16


def contract_last(a, b):
    return lax.dot_general(a, b, (((1,), (1,)), ((), ())), preferred_element_type=F32)


def matmul(a, b):
    return jnp.dot(a, b, preferred_element_type=F32)


def spread_heads(rows, head_size):
    column = lax.broadcasted_iota(jnp.int32, (1, rows.shape[1]), 1) // head_size
    return jnp.concatenate(
        [rows * (column == h).astype(BF16) for h in range(HEADS)], axis=0
    )


def gather_heads(low, high, count, head_size):
    parts = []
    for blended in (low, high):
        width = blended.shape[1] // 2
        column = lax.broadcasted_iota(jnp.int32, (1, width), 1) // head_size
        top = blended[:count, :width]
        bottom = blended[:count, width:]
        for h in range(1, HEADS // 2):
            rows = slice(h * count, (h + 1) * count)
            top = jnp.where(column == h, blended[rows, :width], top)
            bottom = jnp.where(column == h, blended[rows, width:], bottom)
        parts.append(top / bottom)
    return jnp.concatenate(parts, axis=1)


def pack_kernel(features_ref, cols_ref, counts_ref, *refs, sharers):
    slab_refs, (rows_ref, sems, row_sems) = refs[:-3], refs[-3:]
    peers = len(slab_refs)
    _, vert_rows, width = features_ref.shape
    blocks, slots, _ = cols_ref.shape
    extra = rows_ref.shape[1]
    me = lax.axis_index("vert")
    owners = [lax.rem(me + i, peers) // sharers for i in range(peers)]
    copies = []
    for i, slab in enumerate(slab_refs):
        copies.append(
            pltpu.make_async_copy(
                features_ref.at[owners[i]], slab.at[pl.ds(0, vert_rows), :], sems.at[i]
            )
        )
        copies[-1].start()
    lane = lax.broadcasted_iota(jnp.int32, (extra, width), 1)
    for i, slab in enumerate(slab_refs):
        table = jnp.zeros(lane.shape, jnp.int32)
        for b in range(blocks):
            base = b * (slots + 1)
            for t in range(slots):
                table = jnp.where(lane == base + t, cols_ref[b, t, owners[i]], table)
            table = jnp.where(lane == base + slots, counts_ref[b, owners[i]], table)
        rows_ref[i] = table.astype(F32).astype(BF16)
        copies.append(
            pltpu.make_async_copy(
                rows_ref.at[i], slab.at[pl.ds(vert_rows, extra), :], row_sems.at[i]
            )
        )
        copies[-1].start()
    for copy in copies:
        copy.wait()


def pack(features, tile_cols, counts, peers, sharers):
    _, vert_rows, width = features.shape
    smem = pl.BlockSpec(memory_space=pltpu.SMEM)
    hbm = pl.BlockSpec(memory_space=pltpu.HBM)
    slab = jax.ShapeDtypeStruct((vert_rows + EXTRA, width), BF16)
    return list(
        pl.pallas_call(
            functools.partial(pack_kernel, sharers=sharers),
            out_shape=[slab] * peers,
            in_specs=[hbm, smem, smem],
            out_specs=[hbm] * peers,
            scratch_shapes=[
                pltpu.VMEM((peers, EXTRA, width), BF16),
                pltpu.SemaphoreType.DMA((peers,)),
                pltpu.SemaphoreType.DMA((peers,)),
            ],
            name="pack",
        )(
            pltpu.with_memory_space_constraint(features, pltpu.HBM),
            jnp.transpose(tile_cols, (1, 2, 0)),
            counts.T,
        )
    )


def structural_kernel(
    place_ref,
    wk_ref,
    wvt_ref,
    wq_hbm,
    wo_hbm,
    own_hbm,
    *refs,
    slots,
):
    slab_refs, rest = refs[:-14], refs[-14:]
    out_ref, k_ref, v_ref, q_ref, s_ref, p_ref, a_ref, loaded_ref, table_ref = rest[:9]
    table_sem, wq_ref, wo_ref, own_ref, sems = rest[9:]
    fetches = []
    for i, (source, target) in enumerate(((own_hbm, own_ref), (wq_hbm, wq_ref), (wo_hbm, wo_ref))):
        fetches.append(pltpu.make_async_copy(source, target, sems.at[i]))
        fetches[-1].start()
    groups, peers, rows, width = out_ref.shape
    total = k_ref.shape[0]
    vert_rows = total // peers
    quarter = vert_rows // groups
    half = width // 2
    half_heads = HEADS // 2
    head_size = width // HEADS
    blocks = vert_rows // TILE
    row_blocks = total // TILE
    pieces = TILE // quarter
    span = pieces * rows
    lanes = half_heads * span
    units = s_ref.shape[0]
    merged = min(blocks, 128 // span)
    factor = head_size ** (-0.5) * math.log2(math.e)
    offset = pl.multiple_of(place_ref[0], rows)
    senders = [lax.rem(place_ref[1] + peers - i, peers) for i in range(peers)]

    def query_rows(slab):
        return jnp.concatenate(
            [slab[pl.ds(offset + g * quarter, rows), :] for g in range(groups)], axis=0
        )

    def take(sender, slab):
        tail = slab[vert_rows:, :128].astype(F32)
        loaded_ref[pl.ds(sender, 1), :] = tail[:1].astype(jnp.int32)
        at = pl.ds(pl.multiple_of(sender * vert_rows, vert_rows), vert_rows)
        x = slab[:vert_rows, :]
        k_ref[at, :] = matmul(x, wk_ref[...]).astype(BF16)
        values = contract_last(wvt_ref[...], x).astype(BF16)
        v_ref[0, :half, at] = values[:half]
        v_ref[1, :half, at] = values[half:]

    v_ref[:, half:, :total] = jnp.ones((2, v_ref.shape[1] - half, total), BF16)
    v_ref[:, :, total:] = jnp.zeros((2, v_ref.shape[1], TILE), BF16)
    for sender, slab in zip(senders[1:], slab_refs):
        take(sender, slab)
    for fetch in fetches:
        fetch.wait()
    slab_refs = (own_ref, *slab_refs)
    take(senders[0], own_ref)
    load = pltpu.make_async_copy(loaded_ref, table_ref, table_sem)
    load.start()
    for sender, slab in zip(senders, slab_refs):
        queries = (matmul(query_rows(slab), wq_ref[...]) * factor).astype(BF16)
        for g in range(groups):
            q_ref[g, sender] = queries[g * rows : (g + 1) * rows]
    load.wait()

    def read_slots(peer, block):
        base = block * (slots + 1)
        count = table_ref[peer, base + slots]
        first = table_ref[peer, base]
        keys = []
        values = []
        for t in range(slots):
            spot = table_ref[peer, base + t]
            key = jnp.where(count > t, spot, first)
            value = jnp.where(count > t, spot, row_blocks)
            keys.append(pl.ds(pl.multiple_of(key * TILE, TILE), TILE))
            values.append(pl.ds(pl.multiple_of(value * TILE, TILE), TILE))
        return keys, values

    def score(unit, peer, block):
        keys, _ = read_slots(peer, block)
        queries = jnp.concatenate(
            [q_ref[block * pieces + i, peer] for i in range(pieces)], axis=0
        )
        keys = jnp.concatenate([k_ref[key, :] for key in keys], axis=0)
        s_ref[unit] = contract_last(keys, spread_heads(queries, head_size))

    def blend(unit, peer, block):
        _, values = read_slots(peer, block)
        parts = []
        for j in range(2):
            for c in range(j * lanes, (j + 1) * lanes, 128):
                top = jnp.max(s_ref[unit, :, c : c + 128], axis=0, keepdims=True)
                p_ref[unit, :, c : c + 128] = jnp.exp2(
                    s_ref[unit, :, c : c + 128] - top
                ).astype(BF16)
            value = jnp.concatenate([v_ref[j, :, spot] for spot in values], axis=1)
            mixed = matmul(value, p_ref[unit, :, j * lanes : (j + 1) * lanes])
            for h in range(half_heads):
                c = h * span // 128 * 128
                part = mixed[h * head_size : (h + 1) * head_size, c : c + 128]
                part = part / mixed[half : half + 1, c : c + 128]
                shift = (block % merged - h) * span % 128
                if shift:
                    part = pltpu.roll(part, shift, 1)
                parts.append(part)
        return jnp.concatenate(parts, axis=0)

    def some_peers(i, carry):
        todo = [(p, b) for p in range(units // blocks) for b in range(blocks)]
        lane = lax.broadcasted_iota(jnp.int32, (1, 128), 1) // span
        score(0, i * (units // blocks), 0)
        wide = None
        for n, (p, b) in enumerate(todo):
            if n + 1 < len(todo):
                score(n + 1, i * (units // blocks) + todo[n + 1][0], todo[n + 1][1])
            peer = i * (units // blocks) + p
            part = blend(n, peer, b)
            wide = part if b % merged == 0 else jnp.where(lane == b % merged, part, wide)
            if b % merged == merged - 1:
                narrow = wide.T[: merged * span].astype(BF16)
                for n in range(merged * pieces):
                    g = (b + 1 - merged) * pieces + n
                    a_ref[g, peer] = narrow[n * rows : (n + 1) * rows]
        return carry

    lax.fori_loop(0, row_blocks // units, some_peers, 0)
    for sender, slab in zip(senders, slab_refs):
        mixed = jnp.concatenate([a_ref[g, sender] for g in range(groups)], axis=0)
        hidden = query_rows(slab).astype(F32) + matmul(mixed, wo_ref[...])
        for g in range(groups):
            out_ref[g, sender] = hidden[g * rows : (g + 1) * rows].astype(BF16)


def structural(place, slabs, query_proj, keyval_proj, struct_out, vert_rows, rows, groups, slots):
    peers = len(slabs)
    width = slabs[0].shape[1]
    total = peers * vert_rows
    span = TILE // (vert_rows // groups) * rows
    vmem = pl.BlockSpec(memory_space=pltpu.VMEM)
    smem = pl.BlockSpec(memory_space=pltpu.SMEM)
    hbm = pl.BlockSpec(memory_space=pltpu.HBM)
    return pl.pallas_call(
        functools.partial(structural_kernel, slots=slots),
        out_shape=jax.ShapeDtypeStruct((groups, peers, rows, width), BF16),
        in_specs=[smem, vmem, vmem, hbm, hbm, hbm] + [vmem] * (peers - 1),
        out_specs=vmem,
        scratch_shapes=[
            pltpu.VMEM((total, width), BF16),
            pltpu.VMEM((2, width // 2 + 16, total + TILE), BF16),
            pltpu.VMEM((groups, peers, rows, width), BF16),
            pltpu.VMEM((TOGETHER, slots * TILE, HEADS * span), F32),
            pltpu.VMEM((TOGETHER, slots * TILE, HEADS * span), BF16),
            pltpu.VMEM((groups, peers, rows, width), BF16),
            pltpu.VMEM((peers, 128), jnp.int32),
            pltpu.SMEM((peers, 128), jnp.int32),
            pltpu.SemaphoreType.DMA,
            pltpu.VMEM(query_proj.shape, BF16),
            pltpu.VMEM(struct_out.shape, BF16),
            pltpu.VMEM(slabs[0].shape, BF16),
            pltpu.SemaphoreType.DMA((3,)),
        ],
        compiler_params=pltpu.CompilerParams(vmem_limit_bytes=48 * 1024 * 1024),
        name="structural",
    )(
        place,
        keyval_proj[:, :width],
        keyval_proj[:, width:].T,
        *(pltpu.with_memory_space_constraint(a, pltpu.HBM) for a in (query_proj, struct_out)),
        pltpu.with_memory_space_constraint(slabs[0], pltpu.HBM),
        *slabs[1:],
    )


def temporal_kernel(h_ref, birth_ref, pos_ref, wt_ref, wo_ref, *refs):
    out_ref = refs[-1]
    length, count, width = h_ref.shape
    half = width // 2
    head_size = width // HEADS
    factor = head_size ** (-0.5) * math.log2(math.e)
    batch = min(count, 16)
    rows = batch * length
    together = max(1, TILE // length)
    span = together * length
    line = lax.broadcasted_iota(jnp.int32, (rows, rows), 0)
    column = lax.broadcasted_iota(jnp.int32, (rows, rows), 1)
    to_vertex = (
        (line // length == column % batch) & (line % length == column // batch)
    ).astype(BF16)
    to_time = (
        (line % batch == column // length) & (line // batch == column % length)
    ).astype(BF16)
    line = lax.broadcasted_iota(jnp.int32, (span, span), 0)
    column = lax.broadcasted_iota(jnp.int32, (span, span), 1)
    same = line // length == column // length
    before = same & (column < line)
    itself = line == column
    instant = lax.broadcasted_iota(jnp.int32, (1, span), 1) % length
    ones = jnp.ones((span, half), BF16)
    positions = pos_ref[...].astype(F32)[:, None, :]
    for b in range(count // batch):
        part = slice(b * batch, (b + 1) * batch)
        hidden = h_ref[:, part, :].astype(F32)
        time_in = (hidden + positions).astype(BF16).reshape(rows, width)
        time_in = matmul(to_vertex, time_in).astype(BF16)
        projected = matmul(time_in, wt_ref[...]).astype(BF16)
        mixed = []
        for g in range(batch // together):
            at = slice(g * span, (g + 1) * span)
            queries = spread_heads(projected[at, :width], head_size)
            values = projected[at, 2 * width :]
            scores = contract_last(queries, projected[at, width : 2 * width])
            index = b * (batch // together) + g
            alive = instant >= birth_ref[index : index + 1, :]
            kept = itself | (before & alive)
            weights = []
            for h in range(HEADS):
                score = jnp.where(kept, scores[h * span : (h + 1) * span], -jnp.inf)
                top = jnp.max(score, axis=1, keepdims=True)
                weights.append(jnp.exp2((score - top) * factor).astype(BF16))
            low = jnp.concatenate(weights[: HEADS // 2], axis=0)
            high = jnp.concatenate(weights[HEADS // 2 :], axis=0)
            low = matmul(low, jnp.concatenate([values[:, :half], ones], axis=1))
            high = matmul(high, jnp.concatenate([values[:, half:], ones], axis=1))
            mixed.append(gather_heads(low, high, span, head_size).astype(BF16))
        mixed = jnp.concatenate(mixed, axis=0)
        mixed = matmul(to_time, mixed).astype(BF16)
        update = matmul(mixed, wo_ref[...]).reshape(length, batch, width)
        out_ref[:, part, :] = hidden + update


def temporal(hidden, births, positions, qkv_weight, output_weight, total, chunk, earlier):
    length, count, width = hidden.shape
    vmem = pl.BlockSpec(memory_space=pltpu.VMEM)
    args = [hidden, births, positions, qkv_weight, output_weight]
    specs = [pl.BlockSpec(a.shape, lambda i, n=a.ndim: (0,) * n) for a in args]
    aliases = {}
    if earlier is not None:
        aliases = {len(args): 0}
        args.append(earlier)
        specs.append(pl.BlockSpec(memory_space=pl.ANY))
    return pl.pallas_call(
        temporal_kernel,
        grid=(1,),
        out_shape=jax.ShapeDtypeStruct((length, total, width), F32),
        in_specs=specs,
        out_specs=pl.BlockSpec((length, count, width), lambda i: (0, chunk, 0)),
        input_output_aliases=aliases,
        compiler_params=pltpu.CompilerParams(vmem_limit_bytes=48 * 1024 * 1024),
        name="temporal",
    )(*args)


def local(
    features,
    tile_cols,
    counts,
    birth_snap,
    query_proj,
    keyval_proj,
    struct_out,
    position_embedding_table,
    temporal_qkv_weight,
    temporal_output_weight,
):
    snap_count, vert_rows, width = features.shape
    slots = tile_cols.shape[2]
    peers = lax.axis_size("vert")
    groups = lax.axis_size("snap")
    snapshots = snap_count * groups
    quarter = vert_rows // groups
    sharers = peers // snap_count
    chunks = max(1, min(CHUNKS, quarter // (sharers * 16)))
    rows = quarter // (sharers * chunks)

    me = lax.axis_index("vert")
    share = me % sharers
    slabs = pack(features, tile_cols, counts, peers, sharers)
    for i in range(1, peers):
        slabs[i] = lax.ppermute(slabs[i], "vert", [(v, (v + i) % peers) for v in range(peers)])

    arrived = []
    for c in range(chunks):
        place = jnp.stack([(c * sharers + share) * rows, me]).astype(jnp.int32)
        hidden = structural(
            place, slabs, query_proj, keyval_proj, struct_out, vert_rows, rows, groups, slots
        )
        hidden = hidden.reshape(groups * peers, rows, width)
        hidden = lax.all_to_all(
            hidden, ("snap", "vert"), split_axis=0, concat_axis=0, tiled=True
        )
        arrived.append(hidden.reshape(snapshots, sharers * rows, width))

    births = lax.dynamic_slice_in_dim(birth_snap, lax.axis_index("snap") * quarter, quarter)
    span = max(1, TILE // snapshots) * snapshots
    births = jnp.repeat(births, snapshots).reshape(chunks, -1, span)
    result = None
    for c in range(chunks):
        result = temporal(
            arrived[c],
            births[c],
            position_embedding_table,
            temporal_qkv_weight,
            temporal_output_weight,
            quarter,
            c,
            result,
        )
    return result[:, None, None]


def solution(mesh):
    placed = (
        P("snap", "vert", None),
        P("snap", "vert", None),
        P("snap", "vert"),
        P("vert"),
        P(),
        P(),
        P(),
        P(),
        P(),
        P(),
    )
    return jax.shard_map(
        local,
        mesh=mesh,
        in_specs=placed,
        out_specs=P(None, "vert", "snap", None, None),
        check_vma=False,
    )
```

```python
import functools
import math

import jax
import jax.numpy as jnp
from jax import lax
from jax.experimental import pallas as pl
from jax.experimental.pallas import tpu as pltpu
from jax.sharding import PartitionSpec as P

HEADS = 8
TILE = 128
EXTRA = 8
CHUNKS = 2
TOGETHER = 16
F32 = jnp.float32
BF16 = jnp.bfloat16


def contract_last(a, b):
    return lax.dot_general(a, b, (((1,), (1,)), ((), ())), preferred_element_type=F32)


def matmul(a, b):
    return jnp.dot(a, b, preferred_element_type=F32)


def spread_heads(rows, head_size):
    column = lax.broadcasted_iota(jnp.int32, (1, rows.shape[1]), 1) // head_size
    return jnp.concatenate(
        [rows * (column == h).astype(BF16) for h in range(HEADS)], axis=0
    )


def gather_heads(low, high, count, head_size):
    parts = []
    for blended in (low, high):
        width = blended.shape[1] // 2
        column = lax.broadcasted_iota(jnp.int32, (1, width), 1) // head_size
        top = blended[:count, :width]
        bottom = blended[:count, width:]
        for h in range(1, HEADS // 2):
            rows = slice(h * count, (h + 1) * count)
            top = jnp.where(column == h, blended[rows, :width], top)
            bottom = jnp.where(column == h, blended[rows, width:], bottom)
        parts.append(top / bottom)
    return jnp.concatenate(parts, axis=1)


def pack_kernel(features_ref, cols_ref, counts_ref, *refs, sharers):
    slab_refs, (rows_ref, in_sems, out_sems) = refs[:-3], refs[-3:]
    peers = len(slab_refs)
    _, vert_rows, width = features_ref.shape
    blocks, slots, _ = cols_ref.shape
    extra = rows_ref.shape[1] - vert_rows
    me = lax.axis_index("vert")
    owners = [lax.rem(me + i, peers) // sharers for i in range(peers)]
    order = [*range(1, peers), 0]
    arrive = {}
    for i in order:
        arrive[i] = pltpu.make_async_copy(
            features_ref.at[owners[i]], rows_ref.at[i, pl.ds(0, vert_rows), :], in_sems.at[i]
        )
        arrive[i].start()
    lane = lax.broadcasted_iota(jnp.int32, (extra, width), 1)
    for i in order:
        table = jnp.zeros(lane.shape, jnp.int32)
        for b in range(blocks):
            base = b * (slots + 1)
            for t in range(slots):
                table = jnp.where(lane == base + t, cols_ref[b, t, owners[i]], table)
            table = jnp.where(lane == base + slots, counts_ref[b, owners[i]], table)
        rows_ref[i, vert_rows:, :] = table.astype(F32).astype(BF16)
    leave = []
    for i in order:
        arrive[i].wait()
        leave.append(pltpu.make_async_copy(rows_ref.at[i], slab_refs[i], out_sems.at[i]))
        leave[-1].start()
    for copy in leave:
        copy.wait()


def pack(features, tile_cols, counts, peers, sharers):
    _, vert_rows, width = features.shape
    smem = pl.BlockSpec(memory_space=pltpu.SMEM)
    hbm = pl.BlockSpec(memory_space=pltpu.HBM)
    slab = jax.ShapeDtypeStruct((vert_rows + EXTRA, width), BF16)
    return list(
        pl.pallas_call(
            functools.partial(pack_kernel, sharers=sharers),
            out_shape=[slab] * peers,
            in_specs=[hbm, smem, smem],
            out_specs=[hbm] * peers,
            scratch_shapes=[
                pltpu.VMEM((peers, vert_rows + EXTRA, width), BF16),
                pltpu.SemaphoreType.DMA((peers,)),
                pltpu.SemaphoreType.DMA((peers,)),
            ],
            name="pack",
        )(
            pltpu.with_memory_space_constraint(features, pltpu.HBM),
            jnp.transpose(tile_cols, (1, 2, 0)),
            counts.T,
        )
    )


def structural_kernel(
    place_ref,
    wk_ref,
    wvt_ref,
    wq_hbm,
    wo_hbm,
    own_hbm,
    *refs,
    slots,
):
    slab_refs, rest = refs[:-14], refs[-14:]
    out_ref, k_ref, v_ref, q_ref, s_ref, p_ref, a_ref, loaded_ref, table_ref = rest[:9]
    table_sem, wq_ref, wo_ref, own_ref, sems = rest[9:]
    fetches = []
    for i, (source, target) in enumerate(((own_hbm, own_ref), (wq_hbm, wq_ref), (wo_hbm, wo_ref))):
        fetches.append(pltpu.make_async_copy(source, target, sems.at[i]))
        fetches[-1].start()
    groups, peers, rows, width = out_ref.shape
    total = k_ref.shape[0]
    vert_rows = total // peers
    quarter = vert_rows // groups
    half = width // 2
    half_heads = HEADS // 2
    head_size = width // HEADS
    blocks = vert_rows // TILE
    row_blocks = total // TILE
    pieces = TILE // quarter
    span = pieces * rows
    lanes = half_heads * span
    units = s_ref.shape[0]
    merged = min(blocks, 128 // span)
    factor = head_size ** (-0.5) * math.log2(math.e)
    offset = pl.multiple_of(place_ref[0], rows)
    senders = [lax.rem(place_ref[1] + peers - i, peers) for i in range(peers)]

    def query_rows(slab):
        return jnp.concatenate(
            [slab[pl.ds(offset + g * quarter, rows), :] for g in range(groups)], axis=0
        )

    def read_table(sender, slab):
        tail = slab[vert_rows:, :128].astype(F32)
        loaded_ref[pl.ds(sender, 1), :] = tail[:1].astype(jnp.int32)

    def project(sender, slab):
        at = pl.ds(pl.multiple_of(sender * vert_rows, vert_rows), vert_rows)
        x = slab[:vert_rows, :]
        k_ref[at, :] = matmul(x, wk_ref[...]).astype(BF16)
        values = contract_last(wvt_ref[...], x).astype(BF16)
        v_ref[0, :half, at] = values[:half]
        v_ref[1, :half, at] = values[half:]

    v_ref[:, half:, :total] = jnp.ones((2, v_ref.shape[1] - half, total), BF16)
    v_ref[:, :, total:] = jnp.zeros((2, v_ref.shape[1], TILE), BF16)
    slab_refs = (own_ref, *slab_refs)
    early = peers // 2
    for i in range(1, peers):
        read_table(senders[i], slab_refs[i])
    for i in range(1, early):
        project(senders[i], slab_refs[i])
    for fetch in fetches:
        fetch.wait()
    read_table(senders[0], own_ref)
    load = pltpu.make_async_copy(loaded_ref, table_ref, table_sem)
    load.start()
    for i in (*range(early, peers), 0):
        project(senders[i], slab_refs[i])
    for sender, slab in zip(senders, slab_refs):
        queries = (matmul(query_rows(slab), wq_ref[...]) * factor).astype(BF16)
        for g in range(groups):
            q_ref[g, sender] = queries[g * rows : (g + 1) * rows]
    load.wait()

    def read_slots(peer, block):
        base = block * (slots + 1)
        count = table_ref[peer, base + slots]
        first = table_ref[peer, base]
        keys = []
        values = []
        for t in range(slots):
            spot = table_ref[peer, base + t]
            key = jnp.where(count > t, spot, first)
            value = jnp.where(count > t, spot, row_blocks)
            keys.append(pl.ds(pl.multiple_of(key * TILE, TILE), TILE))
            values.append(pl.ds(pl.multiple_of(value * TILE, TILE), TILE))
        return keys, values

    def score(unit, peer, block):
        keys, _ = read_slots(peer, block)
        queries = jnp.concatenate(
            [q_ref[block * pieces + i, peer] for i in range(pieces)], axis=0
        )
        keys = jnp.concatenate([k_ref[key, :] for key in keys], axis=0)
        s_ref[unit] = contract_last(keys, spread_heads(queries, head_size))

    def blend(unit, peer, block):
        _, values = read_slots(peer, block)
        parts = []
        for j in range(2):
            for c in range(j * lanes, (j + 1) * lanes, 128):
                top = jnp.max(s_ref[unit, :, c : c + 128], axis=0, keepdims=True)
                p_ref[unit, :, c : c + 128] = jnp.exp2(
                    s_ref[unit, :, c : c + 128] - top
                ).astype(BF16)
            value = jnp.concatenate([v_ref[j, :, spot] for spot in values], axis=1)
            mixed = matmul(value, p_ref[unit, :, j * lanes : (j + 1) * lanes])
            for h in range(half_heads):
                c = h * span // 128 * 128
                part = mixed[h * head_size : (h + 1) * head_size, c : c + 128]
                part = part / mixed[half : half + 1, c : c + 128]
                shift = (block % merged - h) * span % 128
                if shift:
                    part = pltpu.roll(part, shift, 1)
                parts.append(part)
        return jnp.concatenate(parts, axis=0)

    def some_peers(i, carry):
        todo = [(p, b) for p in range(units // blocks) for b in range(blocks)]
        lane = lax.broadcasted_iota(jnp.int32, (1, 128), 1) // span
        score(0, i * (units // blocks), 0)
        wide = None
        for n, (p, b) in enumerate(todo):
            if n + 1 < len(todo):
                score(n + 1, i * (units // blocks) + todo[n + 1][0], todo[n + 1][1])
            peer = i * (units // blocks) + p
            part = blend(n, peer, b)
            wide = part if b % merged == 0 else jnp.where(lane == b % merged, part, wide)
            if b % merged == merged - 1:
                narrow = wide.T[: merged * span].astype(BF16)
                for n in range(merged * pieces):
                    g = (b + 1 - merged) * pieces + n
                    a_ref[g, peer] = narrow[n * rows : (n + 1) * rows]
        return carry

    lax.fori_loop(0, row_blocks // units, some_peers, 0)
    for sender, slab in zip(senders, slab_refs):
        mixed = jnp.concatenate([a_ref[g, sender] for g in range(groups)], axis=0)
        hidden = query_rows(slab).astype(F32) + matmul(mixed, wo_ref[...])
        for g in range(groups):
            out_ref[g, sender] = hidden[g * rows : (g + 1) * rows].astype(BF16)


def structural(place, slabs, query_proj, keyval_proj, struct_out, vert_rows, rows, groups, slots):
    peers = len(slabs)
    width = slabs[0].shape[1]
    total = peers * vert_rows
    span = TILE // (vert_rows // groups) * rows
    vmem = pl.BlockSpec(memory_space=pltpu.VMEM)
    smem = pl.BlockSpec(memory_space=pltpu.SMEM)
    hbm = pl.BlockSpec(memory_space=pltpu.HBM)
    return pl.pallas_call(
        functools.partial(structural_kernel, slots=slots),
        out_shape=jax.ShapeDtypeStruct((groups, peers, rows, width), BF16),
        in_specs=[smem, vmem, vmem, hbm, hbm, hbm] + [vmem] * (peers - 1),
        out_specs=vmem,
        scratch_shapes=[
            pltpu.VMEM((total, width), BF16),
            pltpu.VMEM((2, width // 2 + 16, total + TILE), BF16),
            pltpu.VMEM((groups, peers, rows, width), BF16),
            pltpu.VMEM((TOGETHER, slots * TILE, HEADS * span), F32),
            pltpu.VMEM((TOGETHER, slots * TILE, HEADS * span), BF16),
            pltpu.VMEM((groups, peers, rows, width), BF16),
            pltpu.VMEM((peers, 128), jnp.int32),
            pltpu.SMEM((peers, 128), jnp.int32),
            pltpu.SemaphoreType.DMA,
            pltpu.VMEM(query_proj.shape, BF16),
            pltpu.VMEM(struct_out.shape, BF16),
            pltpu.VMEM(slabs[0].shape, BF16),
            pltpu.SemaphoreType.DMA((3,)),
        ],
        compiler_params=pltpu.CompilerParams(vmem_limit_bytes=48 * 1024 * 1024),
        name="structural",
    )(
        place,
        keyval_proj[:, :width],
        keyval_proj[:, width:].T,
        *(pltpu.with_memory_space_constraint(a, pltpu.HBM) for a in (query_proj, struct_out)),
        pltpu.with_memory_space_constraint(slabs[0], pltpu.HBM),
        *slabs[1:],
    )


def temporal_kernel(h_ref, birth_ref, pos_ref, wt_ref, wo_ref, *refs):
    out_ref = refs[-1]
    length, count, width = h_ref.shape
    half = width // 2
    head_size = width // HEADS
    factor = head_size ** (-0.5) * math.log2(math.e)
    batch = min(count, 16)
    rows = batch * length
    together = max(1, TILE // length)
    span = together * length
    line = lax.broadcasted_iota(jnp.int32, (rows, rows), 0)
    column = lax.broadcasted_iota(jnp.int32, (rows, rows), 1)
    to_vertex = (
        (line // length == column % batch) & (line % length == column // batch)
    ).astype(BF16)
    to_time = (
        (line % batch == column // length) & (line // batch == column % length)
    ).astype(BF16)
    line = lax.broadcasted_iota(jnp.int32, (span, span), 0)
    column = lax.broadcasted_iota(jnp.int32, (span, span), 1)
    same = line // length == column // length
    before = same & (column < line)
    itself = line == column
    instant = lax.broadcasted_iota(jnp.int32, (1, span), 1) % length
    ones = jnp.ones((span, half), BF16)
    positions = pos_ref[...].astype(F32)[:, None, :]
    for b in range(count // batch):
        part = slice(b * batch, (b + 1) * batch)
        hidden = h_ref[:, part, :].astype(F32)
        time_in = (hidden + positions).astype(BF16).reshape(rows, width)
        time_in = matmul(to_vertex, time_in).astype(BF16)
        projected = matmul(time_in, wt_ref[...]).astype(BF16)
        mixed = []
        for g in range(batch // together):
            at = slice(g * span, (g + 1) * span)
            queries = spread_heads(projected[at, :width], head_size)
            values = projected[at, 2 * width :]
            scores = contract_last(queries, projected[at, width : 2 * width])
            index = b * (batch // together) + g
            alive = instant >= birth_ref[index : index + 1, :]
            kept = itself | (before & alive)
            weights = []
            for h in range(HEADS):
                score = jnp.where(kept, scores[h * span : (h + 1) * span], -jnp.inf)
                top = jnp.max(score, axis=1, keepdims=True)
                weights.append(jnp.exp2((score - top) * factor).astype(BF16))
            low = jnp.concatenate(weights[: HEADS // 2], axis=0)
            high = jnp.concatenate(weights[HEADS // 2 :], axis=0)
            low = matmul(low, jnp.concatenate([values[:, :half], ones], axis=1))
            high = matmul(high, jnp.concatenate([values[:, half:], ones], axis=1))
            mixed.append(gather_heads(low, high, span, head_size).astype(BF16))
        mixed = jnp.concatenate(mixed, axis=0)
        mixed = matmul(to_time, mixed).astype(BF16)
        update = matmul(mixed, wo_ref[...]).reshape(length, batch, width)
        out_ref[:, part, :] = hidden + update


def temporal(hidden, births, positions, qkv_weight, output_weight, total, chunk, earlier):
    length, count, width = hidden.shape
    vmem = pl.BlockSpec(memory_space=pltpu.VMEM)
    args = [hidden, births, positions, qkv_weight, output_weight]
    specs = [pl.BlockSpec(a.shape, lambda i, n=a.ndim: (0,) * n) for a in args]
    aliases = {}
    if earlier is not None:
        aliases = {len(args): 0}
        args.append(earlier)
        specs.append(pl.BlockSpec(memory_space=pl.ANY))
    return pl.pallas_call(
        temporal_kernel,
        grid=(1,),
        out_shape=jax.ShapeDtypeStruct((length, total, width), F32),
        in_specs=specs,
        out_specs=pl.BlockSpec((length, count, width), lambda i: (0, chunk, 0)),
        input_output_aliases=aliases,
        compiler_params=pltpu.CompilerParams(vmem_limit_bytes=48 * 1024 * 1024),
        name="temporal",
    )(*args)


def local(
    features,
    tile_cols,
    counts,
    birth_snap,
    query_proj,
    keyval_proj,
    struct_out,
    position_embedding_table,
    temporal_qkv_weight,
    temporal_output_weight,
):
    snap_count, vert_rows, width = features.shape
    slots = tile_cols.shape[2]
    peers = lax.axis_size("vert")
    groups = lax.axis_size("snap")
    snapshots = snap_count * groups
    quarter = vert_rows // groups
    sharers = peers // snap_count
    chunks = max(1, min(CHUNKS, quarter // (sharers * 16)))
    rows = quarter // (sharers * chunks)

    me = lax.axis_index("vert")
    share = me % sharers
    slabs = pack(features, tile_cols, counts, peers, sharers)
    for i in range(1, peers):
        slabs[i] = lax.ppermute(slabs[i], "vert", [(v, (v + i) % peers) for v in range(peers)])

    arrived = []
    for c in range(chunks):
        place = jnp.stack([(c * sharers + share) * rows, me]).astype(jnp.int32)
        hidden = structural(
            place, slabs, query_proj, keyval_proj, struct_out, vert_rows, rows, groups, slots
        )
        hidden = hidden.reshape(groups * peers, rows, width)
        hidden = lax.all_to_all(
            hidden, ("snap", "vert"), split_axis=0, concat_axis=0, tiled=True
        )
        arrived.append(hidden.reshape(snapshots, sharers * rows, width))

    births = lax.dynamic_slice_in_dim(birth_snap, lax.axis_index("snap") * quarter, quarter)
    span = max(1, TILE // snapshots) * snapshots
    births = jnp.repeat(births, snapshots).reshape(chunks, -1, span)
    result = None
    for c in range(chunks):
        result = temporal(
            arrived[c],
            births[c],
            position_embedding_table,
            temporal_qkv_weight,
            temporal_output_weight,
            quarter,
            c,
            result,
        )
    return result[:, None, None]


def solution(mesh):
    placed = (
        P("snap", "vert", None),
        P("snap", "vert", None),
        P("snap", "vert"),
        P("vert"),
        P(),
        P(),
        P(),
        P(),
        P(),
        P(),
    )
    return jax.shard_map(
        local,
        mesh=mesh,
        in_specs=placed,
        out_specs=P(None, "vert", "snap", None, None),
        check_vma=False,
    )
```

```python
import functools
import math

import jax
import jax.numpy as jnp
from jax import lax
from jax.experimental import pallas as pl
from jax.experimental.pallas import tpu as pltpu
from jax.sharding import PartitionSpec as P

HEADS = 8
TILE = 128
EXTRA = 8
CHUNKS = 2
TOGETHER = 16
F32 = jnp.float32
BF16 = jnp.bfloat16


def contract_last(a, b):
    return lax.dot_general(a, b, (((1,), (1,)), ((), ())), preferred_element_type=F32)


def matmul(a, b):
    return jnp.dot(a, b, preferred_element_type=F32)


def spread_heads(rows, head_size):
    column = lax.broadcasted_iota(jnp.int32, (1, rows.shape[1]), 1) // head_size
    return jnp.concatenate(
        [rows * (column == h).astype(BF16) for h in range(HEADS)], axis=0
    )


def gather_heads(low, high, count, head_size):
    parts = []
    for blended in (low, high):
        width = blended.shape[1] // 2
        column = lax.broadcasted_iota(jnp.int32, (1, width), 1) // head_size
        top = blended[:count, :width]
        bottom = blended[:count, width:]
        for h in range(1, HEADS // 2):
            rows = slice(h * count, (h + 1) * count)
            top = jnp.where(column == h, blended[rows, :width], top)
            bottom = jnp.where(column == h, blended[rows, width:], bottom)
        parts.append(top / bottom)
    return jnp.concatenate(parts, axis=1)


def fill_slab(slab, copy, cols_ref, counts_ref, own, vert_rows):
    copy.start()
    blocks, slots, _ = cols_ref.shape
    lane = lax.broadcasted_iota(jnp.int32, (slab.shape[0] - vert_rows, slab.shape[1]), 1)
    table = jnp.zeros(lane.shape, jnp.int32)
    for b in range(blocks):
        base = b * (slots + 1)
        for t in range(slots):
            table = jnp.where(lane == base + t, cols_ref[b, t, own], table)
        table = jnp.where(lane == base + slots, counts_ref[b, own], table)
    slab[vert_rows:, :] = table.astype(F32).astype(BF16)


def pack_kernel(features_ref, cols_ref, counts_ref, *refs, peers, sharers):
    slab_refs, sems = refs[:-1], refs[-1]
    vert_rows = features_ref.shape[1]
    me = lax.axis_index("vert")
    copies = []
    for i, slab in enumerate(slab_refs):
        own = lax.rem(me + i + 1, peers) // sharers
        features = slab.at[pl.ds(0, vert_rows), :]
        copies.append(pltpu.make_async_copy(features_ref.at[own], features, sems.at[i]))
        fill_slab(slab, copies[-1], cols_ref, counts_ref, own, vert_rows)
    for copy in copies:
        copy.wait()


def stage_kernel(
    features_ref,
    cols_ref,
    counts_ref,
    query_ref,
    keyval_ref,
    struct_ref,
    wq_ref,
    wk_ref,
    wvt_ref,
    wo_ref,
    slab_ref,
    sem,
    *,
    sharers,
):
    vert_rows = features_ref.shape[1]
    width = wq_ref.shape[1]
    own = lax.axis_index("vert") // sharers
    features = slab_ref.at[pl.ds(0, vert_rows), :]
    copy = pltpu.make_async_copy(features_ref.at[own], features, sem)
    fill_slab(slab_ref, copy, cols_ref, counts_ref, own, vert_rows)
    wq_ref[...] = query_ref[...]
    wk_ref[...] = keyval_ref[:, :width]
    wvt_ref[...] = keyval_ref[:, width:].T
    wo_ref[...] = struct_ref[...]
    copy.wait()


def pack(features, tile_cols, counts, query_proj, keyval_proj, struct_out, peers, sharers):
    _, vert_rows, width = features.shape
    smem = pl.BlockSpec(memory_space=pltpu.SMEM)
    hbm = pl.BlockSpec(memory_space=pltpu.HBM)
    vmem = pl.BlockSpec(memory_space=pltpu.VMEM)
    shape = (vert_rows + EXTRA, width)
    fits = 2 * peers * shape[0] * width <= 3 << 19
    slab = pltpu.VMEM(shape, BF16) if fits else jax.ShapeDtypeStruct(shape, BF16)
    tables = (jnp.transpose(tile_cols, (1, 2, 0)), counts.T)
    features = pltpu.with_memory_space_constraint(features, pltpu.HBM)
    slabs = pl.pallas_call(
        functools.partial(pack_kernel, peers=peers, sharers=sharers),
        out_shape=[slab] * (peers - 1),
        in_specs=[hbm, smem, smem],
        out_specs=[vmem] * (peers - 1),
        scratch_shapes=[pltpu.SemaphoreType.DMA((peers - 1,))],
        name="pack",
    )(features, *tables)
    *weights, own = pl.pallas_call(
        functools.partial(stage_kernel, sharers=sharers),
        out_shape=[pltpu.VMEM((width, width), BF16)] * 4 + [pltpu.VMEM(shape, BF16)],
        in_specs=[hbm, smem, smem, vmem, vmem, vmem],
        out_specs=[vmem] * 5,
        scratch_shapes=[pltpu.SemaphoreType.DMA],
        name="stage",
    )(features, *tables, query_proj, keyval_proj, struct_out)
    return [own, *slabs], weights


def structural_kernel(
    place_ref,
    wq_ref,
    wk_ref,
    wvt_ref,
    wo_ref,
    *refs,
    slots,
):
    slab_refs, rest = refs[:-10], refs[-10:]
    out_ref, k_ref, v_ref, q_ref, s_ref, p_ref, a_ref, loaded_ref, table_ref, table_sem = rest
    groups, peers, rows, width = out_ref.shape
    total = k_ref.shape[0]
    vert_rows = total // peers
    quarter = vert_rows // groups
    half = width // 2
    half_heads = HEADS // 2
    head_size = width // HEADS
    blocks = vert_rows // TILE
    row_blocks = total // TILE
    pieces = TILE // quarter
    span = pieces * rows
    lanes = half_heads * span
    units = s_ref.shape[0]
    merged = min(blocks, 128 // span)
    factor = head_size ** (-0.5) * math.log2(math.e)
    offset = pl.multiple_of(place_ref[0], rows)
    senders = [lax.rem(place_ref[1] + peers - i, peers) for i in range(peers)]

    def query_rows(slab):
        return jnp.concatenate(
            [slab[pl.ds(offset + g * quarter, rows), :] for g in range(groups)], axis=0
        )

    def read_table(sender, slab):
        tail = slab[vert_rows:, :128].astype(F32)
        loaded_ref[pl.ds(sender, 1), :] = tail[:1].astype(jnp.int32)

    def project(sender, slab):
        at = pl.ds(pl.multiple_of(sender * vert_rows, vert_rows), vert_rows)
        x = slab[:vert_rows, :]
        k_ref[at, :] = matmul(x, wk_ref[...]).astype(BF16)
        values = contract_last(wvt_ref[...], x).astype(BF16)
        v_ref[0, :half, at] = values[:half]
        v_ref[1, :half, at] = values[half:]

    for sender, slab in zip(senders, slab_refs):
        read_table(sender, slab)
    load = pltpu.make_async_copy(loaded_ref, table_ref, table_sem)
    load.start()
    v_ref[:, half:, :total] = jnp.ones((2, v_ref.shape[1] - half, total), BF16)
    v_ref[:, :, total:] = jnp.zeros((2, v_ref.shape[1], TILE), BF16)
    for sender, slab in zip(senders, slab_refs):
        project(sender, slab)
    for sender, slab in zip(senders, slab_refs):
        queries = (matmul(query_rows(slab), wq_ref[...]) * factor).astype(BF16)
        for g in range(groups):
            q_ref[g, sender] = queries[g * rows : (g + 1) * rows]
    load.wait()

    def read_slots(peer, block):
        base = block * (slots + 1)
        count = table_ref[peer, base + slots]
        first = table_ref[peer, base]
        keys = []
        values = []
        for t in range(slots):
            spot = table_ref[peer, base + t]
            key = jnp.where(count > t, spot, first)
            value = jnp.where(count > t, spot, row_blocks)
            keys.append(pl.ds(pl.multiple_of(key * TILE, TILE), TILE))
            values.append(pl.ds(pl.multiple_of(value * TILE, TILE), TILE))
        return keys, values

    def score(unit, peer, block):
        keys, _ = read_slots(peer, block)
        queries = jnp.concatenate(
            [q_ref[block * pieces + i, peer] for i in range(pieces)], axis=0
        )
        keys = jnp.concatenate([k_ref[key, :] for key in keys], axis=0)
        s_ref[unit] = contract_last(keys, spread_heads(queries, head_size))

    def blend(unit, peer, block):
        _, values = read_slots(peer, block)
        parts = []
        for j in range(2):
            for c in range(j * lanes, (j + 1) * lanes, 128):
                top = jnp.max(s_ref[unit, :, c : c + 128], axis=0, keepdims=True)
                p_ref[unit, :, c : c + 128] = jnp.exp2(
                    s_ref[unit, :, c : c + 128] - top
                ).astype(BF16)
            value = jnp.concatenate([v_ref[j, :, spot] for spot in values], axis=1)
            mixed = matmul(value, p_ref[unit, :, j * lanes : (j + 1) * lanes])
            for h in range(half_heads):
                c = h * span // 128 * 128
                part = mixed[h * head_size : (h + 1) * head_size, c : c + 128]
                part = part / mixed[half : half + 1, c : c + 128]
                shift = (block % merged - h) * span % 128
                if shift:
                    part = pltpu.roll(part, shift, 1)
                parts.append(part)
        return jnp.concatenate(parts, axis=0)

    def some_peers(i, carry):
        todo = [(p, b) for p in range(units // blocks) for b in range(blocks)]
        lane = lax.broadcasted_iota(jnp.int32, (1, 128), 1) // span
        score(0, i * (units // blocks), 0)
        wide = None
        for n, (p, b) in enumerate(todo):
            if n + 1 < len(todo):
                score(n + 1, i * (units // blocks) + todo[n + 1][0], todo[n + 1][1])
            peer = i * (units // blocks) + p
            part = blend(n, peer, b)
            wide = part if b % merged == 0 else jnp.where(lane == b % merged, part, wide)
            if b % merged == merged - 1:
                narrow = wide.T[: merged * span].astype(BF16)
                for n in range(merged * pieces):
                    g = (b + 1 - merged) * pieces + n
                    a_ref[g, peer] = narrow[n * rows : (n + 1) * rows]
        return carry

    lax.fori_loop(0, row_blocks // units, some_peers, 0)
    for sender, slab in zip(senders, slab_refs):
        mixed = jnp.concatenate([a_ref[g, sender] for g in range(groups)], axis=0)
        hidden = query_rows(slab).astype(F32) + matmul(mixed, wo_ref[...])
        for g in range(groups):
            out_ref[g, sender] = hidden[g * rows : (g + 1) * rows].astype(BF16)


def structural(place, slabs, weights, vert_rows, rows, groups, slots):
    peers = len(slabs)
    width = slabs[0].shape[1]
    total = peers * vert_rows
    span = TILE // (vert_rows // groups) * rows
    vmem = pl.BlockSpec(memory_space=pltpu.VMEM)
    smem = pl.BlockSpec(memory_space=pltpu.SMEM)
    return pl.pallas_call(
        functools.partial(structural_kernel, slots=slots),
        out_shape=jax.ShapeDtypeStruct((groups, peers, rows, width), BF16),
        in_specs=[smem] + [vmem] * (4 + peers),
        out_specs=vmem,
        scratch_shapes=[
            pltpu.VMEM((total, width), BF16),
            pltpu.VMEM((2, width // 2 + 16, total + TILE), BF16),
            pltpu.VMEM((groups, peers, rows, width), BF16),
            pltpu.VMEM((TOGETHER, slots * TILE, HEADS * span), F32),
            pltpu.VMEM((TOGETHER, slots * TILE, HEADS * span), BF16),
            pltpu.VMEM((groups, peers, rows, width), BF16),
            pltpu.VMEM((peers, 128), jnp.int32),
            pltpu.SMEM((peers, 128), jnp.int32),
            pltpu.SemaphoreType.DMA,
        ],
        compiler_params=pltpu.CompilerParams(vmem_limit_bytes=48 * 1024 * 1024),
        name="structural",
    )(
        place,
        *weights,
        *slabs,
    )


def temporal_kernel(h_ref, birth_ref, pos_ref, wt_ref, wo_ref, *refs):
    out_ref = refs[-1]
    length, count, width = h_ref.shape
    half = width // 2
    head_size = width // HEADS
    factor = head_size ** (-0.5) * math.log2(math.e)
    batch = min(count, 16)
    rows = batch * length
    together = max(1, TILE // length)
    span = together * length
    line = lax.broadcasted_iota(jnp.int32, (rows, rows), 0)
    column = lax.broadcasted_iota(jnp.int32, (rows, rows), 1)
    to_vertex = (
        (line // length == column % batch) & (line % length == column // batch)
    ).astype(BF16)
    to_time = (
        (line % batch == column // length) & (line // batch == column % length)
    ).astype(BF16)
    line = lax.broadcasted_iota(jnp.int32, (span, span), 0)
    column = lax.broadcasted_iota(jnp.int32, (span, span), 1)
    same = line // length == column // length
    before = same & (column < line)
    itself = line == column
    instant = lax.broadcasted_iota(jnp.int32, (1, span), 1) % length
    ones = jnp.ones((span, half), BF16)
    positions = pos_ref[...].astype(F32)[:, None, :]
    for b in range(count // batch):
        part = slice(b * batch, (b + 1) * batch)
        hidden = h_ref[:, part, :].astype(F32)
        time_in = (hidden + positions).astype(BF16).reshape(rows, width)
        time_in = matmul(to_vertex, time_in).astype(BF16)
        projected = matmul(time_in, wt_ref[...]).astype(BF16)
        mixed = []
        for g in range(batch // together):
            at = slice(g * span, (g + 1) * span)
            queries = spread_heads(projected[at, :width], head_size)
            values = projected[at, 2 * width :]
            scores = contract_last(queries, projected[at, width : 2 * width])
            index = b * (batch // together) + g
            alive = instant >= birth_ref[index : index + 1, :]
            kept = itself | (before & alive)
            weights = []
            for h in range(HEADS):
                score = jnp.where(kept, scores[h * span : (h + 1) * span], -jnp.inf)
                top = jnp.max(score, axis=1, keepdims=True)
                weights.append(jnp.exp2((score - top) * factor).astype(BF16))
            low = jnp.concatenate(weights[: HEADS // 2], axis=0)
            high = jnp.concatenate(weights[HEADS // 2 :], axis=0)
            low = matmul(low, jnp.concatenate([values[:, :half], ones], axis=1))
            high = matmul(high, jnp.concatenate([values[:, half:], ones], axis=1))
            mixed.append(gather_heads(low, high, span, head_size).astype(BF16))
        mixed = jnp.concatenate(mixed, axis=0)
        mixed = matmul(to_time, mixed).astype(BF16)
        update = matmul(mixed, wo_ref[...]).reshape(length, batch, width)
        out_ref[:, part, :] = hidden + update


def temporal(hidden, births, positions, qkv_weight, output_weight, total, chunk, earlier):
    length, count, width = hidden.shape
    vmem = pl.BlockSpec(memory_space=pltpu.VMEM)
    args = [hidden, births, positions, qkv_weight, output_weight]
    specs = [pl.BlockSpec(a.shape, lambda i, n=a.ndim: (0,) * n) for a in args]
    aliases = {}
    if earlier is not None:
        aliases = {len(args): 0}
        args.append(earlier)
        specs.append(pl.BlockSpec(memory_space=pl.ANY))
    return pl.pallas_call(
        temporal_kernel,
        grid=(1,),
        out_shape=jax.ShapeDtypeStruct((length, total, width), F32),
        in_specs=specs,
        out_specs=pl.BlockSpec((length, count, width), lambda i: (0, chunk, 0)),
        input_output_aliases=aliases,
        compiler_params=pltpu.CompilerParams(vmem_limit_bytes=48 * 1024 * 1024),
        name="temporal",
    )(*args)


def local(
    features,
    tile_cols,
    counts,
    birth_snap,
    query_proj,
    keyval_proj,
    struct_out,
    position_embedding_table,
    temporal_qkv_weight,
    temporal_output_weight,
):
    snap_count, vert_rows, width = features.shape
    slots = tile_cols.shape[2]
    peers = lax.axis_size("vert")
    groups = lax.axis_size("snap")
    snapshots = snap_count * groups
    quarter = vert_rows // groups
    sharers = peers // snap_count
    chunks = max(1, min(CHUNKS, quarter // (sharers * 16)))
    rows = quarter // (sharers * chunks)

    me = lax.axis_index("vert")
    share = me % sharers
    slabs, weights = pack(
        features, tile_cols, counts, query_proj, keyval_proj, struct_out, peers, sharers
    )
    for i in range(1, peers):
        slabs[i] = lax.ppermute(slabs[i], "vert", [(v, (v + i) % peers) for v in range(peers)])

    arrived = []
    for c in range(chunks):
        place = jnp.stack([(c * sharers + share) * rows, me]).astype(jnp.int32)
        hidden = structural(place, slabs, weights, vert_rows, rows, groups, slots)
        hidden = hidden.reshape(groups * peers, rows, width)
        hidden = lax.all_to_all(
            hidden, ("snap", "vert"), split_axis=0, concat_axis=0, tiled=True
        )
        arrived.append(hidden.reshape(snapshots, sharers * rows, width))

    births = lax.dynamic_slice_in_dim(birth_snap, lax.axis_index("snap") * quarter, quarter)
    span = max(1, TILE // snapshots) * snapshots
    births = jnp.repeat(births, snapshots).reshape(chunks, -1, span)
    result = None
    for c in range(chunks):
        result = temporal(
            arrived[c],
            births[c],
            position_embedding_table,
            temporal_qkv_weight,
            temporal_output_weight,
            quarter,
            c,
            result,
        )
    return result[:, None, None]


def solution(mesh):
    placed = (
        P("snap", "vert", None),
        P("snap", "vert", None),
        P("snap", "vert"),
        P("vert"),
        P(),
        P(),
        P(),
        P(),
        P(),
        P(),
    )
    return jax.shard_map(
        local,
        mesh=mesh,
        in_specs=placed,
        out_specs=P(None, "vert", "snap", None, None),
        check_vma=False,
    )
```

```python
import functools
import math

import jax
import jax.numpy as jnp
from jax import lax
from jax.experimental import pallas as pl
from jax.experimental.pallas import tpu as pltpu
from jax.sharding import PartitionSpec as P

HEADS = 8
TILE = 128
EXTRA = 8
CHUNKS = 2
TOGETHER = 16
F32 = jnp.float32
BF16 = jnp.bfloat16


def contract_last(a, b):
    return lax.dot_general(a, b, (((1,), (1,)), ((), ())), preferred_element_type=F32)


def matmul(a, b):
    return jnp.dot(a, b, preferred_element_type=F32)


def spread_heads(rows, head_size):
    column = lax.broadcasted_iota(jnp.int32, (1, rows.shape[1]), 1) // head_size
    return jnp.concatenate(
        [rows * (column == h).astype(BF16) for h in range(HEADS)], axis=0
    )


def gather_heads(low, high, count, head_size):
    parts = []
    for blended in (low, high):
        width = blended.shape[1] // 2
        column = lax.broadcasted_iota(jnp.int32, (1, width), 1) // head_size
        top = blended[:count, :width]
        bottom = blended[:count, width:]
        for h in range(1, HEADS // 2):
            rows = slice(h * count, (h + 1) * count)
            top = jnp.where(column == h, blended[rows, :width], top)
            bottom = jnp.where(column == h, blended[rows, width:], bottom)
        parts.append(top / bottom)
    return jnp.concatenate(parts, axis=1)


def fill_slab(slab, copy, cols_ref, counts_ref, own, vert_rows):
    copy.start()
    blocks, slots, _ = cols_ref.shape
    lane = lax.broadcasted_iota(jnp.int32, (slab.shape[0] - vert_rows, slab.shape[1]), 1)
    table = jnp.zeros(lane.shape, jnp.int32)
    for b in range(blocks):
        base = b * (slots + 1)
        for t in range(slots):
            table = jnp.where(lane == base + t, cols_ref[b, t, own], table)
        table = jnp.where(lane == base + slots, counts_ref[b, own], table)
    slab[vert_rows:, :] = table.astype(F32).astype(BF16)


def pack_kernel(features_ref, cols_ref, counts_ref, *refs, peers, sharers):
    slab_refs, sems = refs[:-1], refs[-1]
    vert_rows = features_ref.shape[1]
    me = lax.axis_index("vert")
    copies = []
    for i, slab in enumerate(slab_refs):
        own = lax.rem(me + peers - i - 1, peers) // sharers
        features = slab.at[pl.ds(0, vert_rows), :]
        copies.append(pltpu.make_async_copy(features_ref.at[own], features, sems.at[i]))
        fill_slab(slab, copies[-1], cols_ref, counts_ref, own, vert_rows)
    for copy in copies:
        copy.wait()


def stage_kernel(
    features_ref,
    cols_ref,
    counts_ref,
    query_ref,
    keyval_ref,
    struct_ref,
    wq_ref,
    wk_ref,
    wvt_ref,
    wo_ref,
    slab_ref,
    sem,
    *,
    sharers,
):
    vert_rows = features_ref.shape[1]
    width = wq_ref.shape[1]
    own = lax.axis_index("vert") // sharers
    features = slab_ref.at[pl.ds(0, vert_rows), :]
    copy = pltpu.make_async_copy(features_ref.at[own], features, sem)
    fill_slab(slab_ref, copy, cols_ref, counts_ref, own, vert_rows)
    wq_ref[...] = query_ref[...]
    wk_ref[...] = keyval_ref[:, :width]
    wvt_ref[...] = keyval_ref[:, width:].T
    wo_ref[...] = struct_ref[...]
    copy.wait()


def pack(features, tile_cols, counts, query_proj, keyval_proj, struct_out, peers, sharers):
    _, vert_rows, width = features.shape
    smem = pl.BlockSpec(memory_space=pltpu.SMEM)
    hbm = pl.BlockSpec(memory_space=pltpu.HBM)
    vmem = pl.BlockSpec(memory_space=pltpu.VMEM)
    shape = (vert_rows + EXTRA, width)
    fits = 2 * peers * shape[0] * width <= 3 << 19
    slab = pltpu.VMEM(shape, BF16) if fits else jax.ShapeDtypeStruct(shape, BF16)
    tables = (jnp.transpose(tile_cols, (1, 2, 0)), counts.T)
    features = pltpu.with_memory_space_constraint(features, pltpu.HBM)
    slabs = pl.pallas_call(
        functools.partial(pack_kernel, peers=peers, sharers=sharers),
        out_shape=[slab] * (peers - 1),
        in_specs=[hbm, smem, smem],
        out_specs=[vmem] * (peers - 1),
        scratch_shapes=[pltpu.SemaphoreType.DMA((peers - 1,))],
        name="pack",
    )(features, *tables)
    *weights, own = pl.pallas_call(
        functools.partial(stage_kernel, sharers=sharers),
        out_shape=[pltpu.VMEM((width, width), BF16)] * 4 + [pltpu.VMEM(shape, BF16)],
        in_specs=[hbm, smem, smem, vmem, vmem, vmem],
        out_specs=[vmem] * 5,
        scratch_shapes=[pltpu.SemaphoreType.DMA],
        name="stage",
    )(features, *tables, query_proj, keyval_proj, struct_out)
    return [own, *slabs], weights


def structural_kernel(
    place_ref,
    wq_ref,
    wk_ref,
    wvt_ref,
    wo_ref,
    *refs,
    slots,
):
    slab_refs, rest = refs[:-10], refs[-10:]
    out_ref, k_ref, v_ref, q_ref, s_ref, p_ref, a_ref, loaded_ref, table_ref, table_sem = rest
    groups, peers, rows, width = out_ref.shape
    total = k_ref.shape[0]
    vert_rows = total // peers
    quarter = vert_rows // groups
    half = width // 2
    half_heads = HEADS // 2
    head_size = width // HEADS
    blocks = vert_rows // TILE
    row_blocks = total // TILE
    pieces = TILE // quarter
    span = pieces * rows
    lanes = half_heads * span
    units = s_ref.shape[0]
    merged = min(blocks, 128 // span)
    factor = head_size ** (-0.5) * math.log2(math.e)
    offset = pl.multiple_of(place_ref[0], rows)
    senders = [lax.rem(place_ref[1] + i, peers) for i in range(peers)]

    def query_rows(slab):
        return jnp.concatenate(
            [slab[pl.ds(offset + g * quarter, rows), :] for g in range(groups)], axis=0
        )

    def read_table(sender, slab):
        tail = slab[vert_rows:, :128].astype(F32)
        loaded_ref[pl.ds(sender, 1), :] = tail[:1].astype(jnp.int32)

    def project(sender, slab):
        at = pl.ds(pl.multiple_of(sender * vert_rows, vert_rows), vert_rows)
        x = slab[:vert_rows, :]
        k_ref[at, :] = matmul(x, wk_ref[...]).astype(BF16)
        values = contract_last(wvt_ref[...], x).astype(BF16)
        v_ref[0, :half, at] = values[:half]
        v_ref[1, :half, at] = values[half:]

    for sender, slab in zip(senders, slab_refs):
        read_table(sender, slab)
    load = pltpu.make_async_copy(loaded_ref, table_ref, table_sem)
    load.start()
    v_ref[:, half:, :total] = jnp.ones((2, v_ref.shape[1] - half, total), BF16)
    v_ref[:, :, total:] = jnp.zeros((2, v_ref.shape[1], TILE), BF16)
    for sender, slab in zip(senders, slab_refs):
        project(sender, slab)
    for sender, slab in zip(senders, slab_refs):
        queries = (matmul(query_rows(slab), wq_ref[...]) * factor).astype(BF16)
        for g in range(groups):
            q_ref[g, sender] = queries[g * rows : (g + 1) * rows]
    load.wait()

    def read_slots(peer, block):
        base = block * (slots + 1)
        count = table_ref[peer, base + slots]
        first = table_ref[peer, base]
        keys = []
        values = []
        for t in range(slots):
            spot = table_ref[peer, base + t]
            key = jnp.where(count > t, spot, first)
            value = jnp.where(count > t, spot, row_blocks)
            keys.append(pl.ds(pl.multiple_of(key * TILE, TILE), TILE))
            values.append(pl.ds(pl.multiple_of(value * TILE, TILE), TILE))
        return keys, values

    def score(unit, peer, block):
        keys, _ = read_slots(peer, block)
        queries = jnp.concatenate(
            [q_ref[block * pieces + i, peer] for i in range(pieces)], axis=0
        )
        keys = jnp.concatenate([k_ref[key, :] for key in keys], axis=0)
        s_ref[unit] = contract_last(keys, spread_heads(queries, head_size))

    def blend(unit, peer, block):
        _, values = read_slots(peer, block)
        parts = []
        for j in range(2):
            for c in range(j * lanes, (j + 1) * lanes, 128):
                top = jnp.max(s_ref[unit, :, c : c + 128], axis=0, keepdims=True)
                p_ref[unit, :, c : c + 128] = jnp.exp2(
                    s_ref[unit, :, c : c + 128] - top
                ).astype(BF16)
            value = jnp.concatenate([v_ref[j, :, spot] for spot in values], axis=1)
            mixed = matmul(value, p_ref[unit, :, j * lanes : (j + 1) * lanes])
            for h in range(half_heads):
                c = h * span // 128 * 128
                part = mixed[h * head_size : (h + 1) * head_size, c : c + 128]
                part = part / mixed[half : half + 1, c : c + 128]
                shift = (block % merged - h) * span % 128
                if shift:
                    part = pltpu.roll(part, shift, 1)
                parts.append(part)
        return jnp.concatenate(parts, axis=0)

    def some_peers(i, carry):
        todo = [(p, b) for p in range(units // blocks) for b in range(blocks)]
        lane = lax.broadcasted_iota(jnp.int32, (1, 128), 1) // span
        score(0, i * (units // blocks), 0)
        wide = None
        for n, (p, b) in enumerate(todo):
            if n + 1 < len(todo):
                score(n + 1, i * (units // blocks) + todo[n + 1][0], todo[n + 1][1])
            peer = i * (units // blocks) + p
            part = blend(n, peer, b)
            wide = part if b % merged == 0 else jnp.where(lane == b % merged, part, wide)
            if b % merged == merged - 1:
                narrow = wide.T[: merged * span].astype(BF16)
                for n in range(merged * pieces):
                    g = (b + 1 - merged) * pieces + n
                    a_ref[g, peer] = narrow[n * rows : (n + 1) * rows]
        return carry

    lax.fori_loop(0, row_blocks // units, some_peers, 0)
    for sender, slab in zip(senders, slab_refs):
        mixed = jnp.concatenate([a_ref[g, sender] for g in range(groups)], axis=0)
        hidden = query_rows(slab).astype(F32) + matmul(mixed, wo_ref[...])
        for g in range(groups):
            out_ref[g, sender] = hidden[g * rows : (g + 1) * rows].astype(BF16)


def structural(place, slabs, weights, vert_rows, rows, groups, slots):
    peers = len(slabs)
    width = slabs[0].shape[1]
    total = peers * vert_rows
    span = TILE // (vert_rows // groups) * rows
    vmem = pl.BlockSpec(memory_space=pltpu.VMEM)
    smem = pl.BlockSpec(memory_space=pltpu.SMEM)
    return pl.pallas_call(
        functools.partial(structural_kernel, slots=slots),
        out_shape=jax.ShapeDtypeStruct((groups, peers, rows, width), BF16),
        in_specs=[smem] + [vmem] * (4 + peers),
        out_specs=vmem,
        scratch_shapes=[
            pltpu.VMEM((total, width), BF16),
            pltpu.VMEM((2, width // 2 + 16, total + TILE), BF16),
            pltpu.VMEM((groups, peers, rows, width), BF16),
            pltpu.VMEM((TOGETHER, slots * TILE, HEADS * span), F32),
            pltpu.VMEM((TOGETHER, slots * TILE, HEADS * span), BF16),
            pltpu.VMEM((groups, peers, rows, width), BF16),
            pltpu.VMEM((peers, 128), jnp.int32),
            pltpu.SMEM((peers, 128), jnp.int32),
            pltpu.SemaphoreType.DMA,
        ],
        compiler_params=pltpu.CompilerParams(vmem_limit_bytes=48 * 1024 * 1024),
        name="structural",
    )(
        place,
        *weights,
        *slabs,
    )


def temporal_kernel(h_ref, birth_ref, pos_ref, wt_ref, wo_ref, *refs):
    out_ref = refs[-1]
    length, count, width = h_ref.shape
    half = width // 2
    head_size = width // HEADS
    factor = head_size ** (-0.5) * math.log2(math.e)
    batch = min(count, 16)
    rows = batch * length
    together = max(1, TILE // length)
    span = together * length
    line = lax.broadcasted_iota(jnp.int32, (rows, rows), 0)
    column = lax.broadcasted_iota(jnp.int32, (rows, rows), 1)
    to_vertex = (
        (line // length == column % batch) & (line % length == column // batch)
    ).astype(BF16)
    to_time = (
        (line % batch == column // length) & (line // batch == column % length)
    ).astype(BF16)
    line = lax.broadcasted_iota(jnp.int32, (span, span), 0)
    column = lax.broadcasted_iota(jnp.int32, (span, span), 1)
    same = line // length == column // length
    before = same & (column < line)
    itself = line == column
    instant = lax.broadcasted_iota(jnp.int32, (1, span), 1) % length
    ones = jnp.ones((span, half), BF16)
    positions = pos_ref[...].astype(F32)[:, None, :]
    for b in range(count // batch):
        part = slice(b * batch, (b + 1) * batch)
        hidden = h_ref[:, part, :].astype(F32)
        time_in = (hidden + positions).astype(BF16).reshape(rows, width)
        time_in = matmul(to_vertex, time_in).astype(BF16)
        projected = matmul(time_in, wt_ref[...]).astype(BF16)
        mixed = []
        for g in range(batch // together):
            at = slice(g * span, (g + 1) * span)
            queries = spread_heads(projected[at, :width], head_size)
            values = projected[at, 2 * width :]
            scores = contract_last(queries, projected[at, width : 2 * width])
            index = b * (batch // together) + g
            alive = instant >= birth_ref[index : index + 1, :]
            kept = itself | (before & alive)
            weights = []
            for h in range(HEADS):
                score = jnp.where(kept, scores[h * span : (h + 1) * span], -jnp.inf)
                top = jnp.max(score, axis=1, keepdims=True)
                weights.append(jnp.exp2((score - top) * factor).astype(BF16))
            low = jnp.concatenate(weights[: HEADS // 2], axis=0)
            high = jnp.concatenate(weights[HEADS // 2 :], axis=0)
            low = matmul(low, jnp.concatenate([values[:, :half], ones], axis=1))
            high = matmul(high, jnp.concatenate([values[:, half:], ones], axis=1))
            mixed.append(gather_heads(low, high, span, head_size).astype(BF16))
        mixed = jnp.concatenate(mixed, axis=0)
        mixed = matmul(to_time, mixed).astype(BF16)
        update = matmul(mixed, wo_ref[...]).reshape(length, batch, width)
        out_ref[:, part, :] = hidden + update


def temporal(hidden, births, positions, qkv_weight, output_weight, total, chunk, earlier):
    length, count, width = hidden.shape
    vmem = pl.BlockSpec(memory_space=pltpu.VMEM)
    args = [hidden, births, positions, qkv_weight, output_weight]
    specs = [pl.BlockSpec(a.shape, lambda i, n=a.ndim: (0,) * n) for a in args]
    aliases = {}
    if earlier is not None:
        aliases = {len(args): 0}
        args.append(earlier)
        specs.append(pl.BlockSpec(memory_space=pl.ANY))
    return pl.pallas_call(
        temporal_kernel,
        grid=(1,),
        out_shape=jax.ShapeDtypeStruct((length, total, width), F32),
        in_specs=specs,
        out_specs=pl.BlockSpec((length, count, width), lambda i: (0, chunk, 0)),
        input_output_aliases=aliases,
        compiler_params=pltpu.CompilerParams(vmem_limit_bytes=48 * 1024 * 1024),
        name="temporal",
    )(*args)


def local(
    features,
    tile_cols,
    counts,
    birth_snap,
    query_proj,
    keyval_proj,
    struct_out,
    position_embedding_table,
    temporal_qkv_weight,
    temporal_output_weight,
):
    snap_count, vert_rows, width = features.shape
    slots = tile_cols.shape[2]
    peers = lax.axis_size("vert")
    groups = lax.axis_size("snap")
    snapshots = snap_count * groups
    quarter = vert_rows // groups
    sharers = peers // snap_count
    chunks = max(1, min(CHUNKS, quarter // (sharers * 16)))
    rows = quarter // (sharers * chunks)

    me = lax.axis_index("vert")
    share = me % sharers
    slabs, weights = pack(
        features, tile_cols, counts, query_proj, keyval_proj, struct_out, peers, sharers
    )
    for i in range(1, peers):
        slabs[i] = lax.ppermute(slabs[i], "vert", [(v, (v - i) % peers) for v in range(peers)])

    arrived = []
    for c in range(chunks):
        place = jnp.stack([(c * sharers + share) * rows, me]).astype(jnp.int32)
        hidden = structural(place, slabs, weights, vert_rows, rows, groups, slots)
        hidden = hidden.reshape(groups * peers, rows, width)
        hidden = lax.all_to_all(
            hidden, ("snap", "vert"), split_axis=0, concat_axis=0, tiled=True
        )
        arrived.append(hidden.reshape(snapshots, sharers * rows, width))

    births = lax.dynamic_slice_in_dim(birth_snap, lax.axis_index("snap") * quarter, quarter)
    span = max(1, TILE // snapshots) * snapshots
    births = jnp.repeat(births, snapshots).reshape(chunks, -1, span)
    result = None
    for c in range(chunks):
        result = temporal(
            arrived[c],
            births[c],
            position_embedding_table,
            temporal_qkv_weight,
            temporal_output_weight,
            quarter,
            c,
            result,
        )
    return result[:, None, None]


def solution(mesh):
    placed = (
        P("snap", "vert", None),
        P("snap", "vert", None),
        P("snap", "vert"),
        P("vert"),
        P(),
        P(),
        P(),
        P(),
        P(),
        P(),
    )
    return jax.shard_map(
        local,
        mesh=mesh,
        in_specs=placed,
        out_specs=P(None, "vert", "snap", None, None),
        check_vma=False,
    )
```
